256 devices in a mesh: row: 8 (over y, core), col: 8 (over z), depth: 4 (over x).
Axes of the slice: x: 4, y: 4, z: 8, core: 2. Of those that a mesh axis runs over, the one named last changes fastest.
Arguments:
- matrix: float32 [4, 8, 512, 16384], P(None, 'row', None, ('col', 'depth')), as said below
Outputs:
- factored: float32 [4, 8, 512, 16384], P(None, 'row', None, ('col', 'depth'))
Inputs may be any that keep to these rules, and one draw needn't show every extreme that they name: matrix is symmetric positive definite.
All inputs are finite; a program needn't handle non-finite values.
Results may differ from the reference program's by a relative error of at most 0.0001.
Values sent between devices are 32-bit elements; how exact they have to be, the bound alone decides.
A program may use at most 128 MiB of HBM per device.

```python
import math
import jax
import jax.numpy as jnp
from jax import lax

B = 512
PANELS = 2
RB = 4
NBLK = 32
ORDER = 16384
N_ROW = 8


def draw_matrix(key, part):
    key_normal = jax.random.fold_in(key, 11)
    key_diagonal = jax.random.fold_in(key, 12)
    latent = 4 * B
    gaussian = jax.random.normal(key_normal, (ORDER, latent), jnp.float32)
    product = jnp.dot(gaussian, gaussian.T, precision=lax.Precision.HIGHEST) / math.sqrt(latent)
    symmetric = (product + product.T) * 0.5
    diag_shift = jax.random.uniform(key_diagonal, (ORDER,), jnp.float32, 0.1, 0.3) * math.sqrt(latent)
    positions = jnp.arange(ORDER)
    symmetric = symmetric.at[positions, positions].add(diag_shift)
    return symmetric.reshape(RB, N_ROW, B, ORDER)


def setup_inputs(seed: int = 0) -> dict:
    seeds = jax.random.split(jax.random.key(seed), 2)
    return {
        "matrix": draw_matrix(jax.random.fold_in(seeds[1], 71), 0),
    }


def factor_blocks(lower_factor, blocks, block_ids, panel_index):
    count_rows, block_size, _ = blocks.shape
    solved = lax.linalg.triangular_solve(lower_factor, blocks.reshape(count_rows * block_size, block_size), left_side=False, lower=True, transpose_a=True)
    solved = solved.reshape(count_rows, block_size, block_size)
    marks = block_ids[:, None, None]
    return jnp.where(marks > panel_index, solved, jnp.where(marks == panel_index, lower_factor[None], jnp.float32(0.0)))

def reference(matrix):
    matrix_full = matrix.reshape(ORDER, ORDER)
    for panel_index in range(PANELS):
        start_col = panel_index * B
        stop_col = start_col + B
        lower_factor = jnp.linalg.cholesky(matrix_full[start_col:stop_col, start_col:stop_col])
        blocks = matrix_full[:, start_col:stop_col].reshape(NBLK, B, B)
        panel_full = factor_blocks(lower_factor, blocks, jnp.arange(NBLK, dtype=jnp.int32), panel_index).reshape(ORDER, B)
        trailing = matrix_full[:, stop_col:] - jnp.dot(panel_full, panel_full[stop_col:].T, precision=lax.Precision.HIGHEST)
        below_rows = (jnp.arange(ORDER, dtype=jnp.int32) >= stop_col)[:, None]
        trailing = jnp.where(below_rows, trailing, jnp.float32(0.0))
        matrix_full = jnp.concatenate([matrix_full[:, :start_col], panel_full, trailing], axis=1)
    return matrix_full.reshape(RB, N_ROW, B, ORDER)
```

```python
import functools
import jax
import jax.numpy as jnp
from jax import lax
from jax.experimental import pallas as pl
from jax.experimental.pallas import tpu as pltpu
from jax.sharding import PartitionSpec as P

HI = lax.Precision.HIGHEST
F32 = jnp.float32
BF16 = jnp.bfloat16
MESH = pl.DeviceIdType.MESH
B = 512
ROW_SPLIT = 24
NS = 16
Z_ORDER = (0, 1, 7, 2, 6, 3, 5, 4)

R_TS = 0
R_CR = 4
R_CS = 12
R_A0 = 20
R_A1 = 36
R_A2 = 44
R_P1Z = 52
R_P1X = 60
R_P2X = 64
R_P2Z = 96
N_RECV = 128
S_TS = 0
S_CR = 16
S_CS = 24
S_A = 32
S_P1Z = 256
S_P1X = 264
S_P2X = 268
S_P2Z = 300
N_SEND = 332


class Comm:
    def __init__(self, m_ref, tbuf, cbuf, abuf, ssem, rsem, lsem):
        self.m, self.t, self.c, self.a = m_ref, tbuf, cbuf, abuf
        self.ssem, self.rsem, self.lsem = ssem, rsem, lsem
        self.r = lax.axis_index("row")
        self.z = lax.axis_index("col")
        self.x = lax.axis_index("depth")
        self.y = self.r // 2
        self.k = self.r % 2
        self.q = self.z * 4 + self.x
        self.other = self.coord(row=self.r + 1 - 2 * self.k)

    def coord(self, row=None, z=None, x=None):
        return {
            "row": self.r if row is None else row,
            "col": self.z if z is None else z,
            "depth": self.x if x is None else x,
        }

    def remote(self, src, dst, ssem, rsem, to):
        return pltpu.make_async_remote_copy(
            src_ref=src,
            dst_ref=dst,
            send_sem=self.ssem.at[ssem],
            recv_sem=self.rsem.at[rsem],
            device_id=to,
            device_id_type=MESH,
        )

    def wait_recv(self, ref, rsem):
        self.remote(ref, ref, 0, rsem, self.other).wait_recv()

    def wait_send(self, ref, ssem):
        self.remote(ref, ref, ssem, 0, self.other).wait_send()

    def barrier(self):
        sem = pltpu.get_barrier_semaphore()
        r, z, x, y, k, q = self.r, self.z, self.x, self.y, self.k, self.q
        ring = [
            self.coord(row=r + 1 - 2 * k),
            self.coord(row=(r + 2) % 8),
            self.coord(row=(r + 6) % 8),
            self.coord(z=(z + 1) % 8),
            self.coord(z=(z + 7) % 8),
            self.coord(x=(x + 1) % 4),
            self.coord(x=(x + 3) % 4),
        ]
        for to in ring:
            pl.semaphore_signal(sem, inc=1, device_id=to, device_id_type=MESH)
        mine = r == q // 16
        for a in range(4):
            col = 8 * a + r

            @pl.when(jnp.logical_not(mine & (col == q)))
            def _():
                to = self.coord(row=q // 16, z=col // 4, x=col % 4)
                pl.semaphore_signal(sem, inc=1, device_id=to, device_id_type=MESH)

        source = r < 2
        dest = q % 8

        @pl.when(source)
        def _():
            def one(i, carry):
                p = r * 16 + i

                @pl.when(jnp.logical_not((dest == r) & (p == q)))
                def _():
                    to = self.coord(row=dest, z=p // 4, x=p % 4)
                    pl.semaphore_signal(sem, inc=1, device_id=to, device_id_type=MESH)

                return carry

            lax.fori_loop(0, 16, one, 0)

        self.own = mine & (q % 8 == r)
        own = self.own.astype(jnp.int32)
        pl.semaphore_wait(sem, 11 - own + source.astype(jnp.int32) * (16 - own))

    def chunk_c(self, k, i):
        return self.c.at[pl.ds(pl.multiple_of(k * B + i * 64, 64), 64), :]

    def load(self):
        @pl.when(self.r < 2)
        def _():
            dst = self.c.at[pl.ds(pl.multiple_of(self.k * B, B), B), :]
            cp = pltpu.make_async_copy(self.m.at[0, 0], dst, self.lsem.at[0])
            cp.start()
            for b, (xs, ks) in enumerate(((0, 0), (1, 0), (1, 1))):

                @pl.when((self.z == 0) & (self.x == xs) & (self.k == ks))
                def _():
                    ca = pltpu.make_async_copy(self.m.at[0, 0], self.a.at[b], self.lsem.at[1])
                    ca.start()
                    ca.wait()

            cp.wait()

    def ts_piece(self, p, a):
        return self.t.at[pl.ds(pl.multiple_of(p * 32, 32), 32), pl.ds(pl.multiple_of(a * B, B), B)]

    def ts_send(self):
        @pl.when(self.r < 2)
        def _():
            dest = self.q % 8
            a = self.q // 8

            def one(i, carry):
                p = self.r * 16 + i
                src = self.c.at[pl.ds(pl.multiple_of(p * 32, 32), 32), :]
                dst = self.ts_piece(p, a)
                is_own = (dest == self.r) & (p == self.q)

                @pl.when(jnp.logical_not(is_own))
                def _():
                    to = self.coord(row=dest, z=p // 4, x=p % 4)
                    self.remote(src, dst, S_TS + i, R_TS + a, to).start()

                @pl.when(is_own)
                def _():
                    pltpu.make_async_copy(src, dst, self.lsem.at[2]).start()

                return carry

            lax.fori_loop(0, 16, one, 0)

    def ts_wait(self):
        for a in range(4):
            own = self.own & (self.q // 8 == a)

            @pl.when(jnp.logical_not(own))
            def _():
                self.wait_recv(self.ts_piece(self.q, a), R_TS + a)

            @pl.when(own)
            def _():
                ref = self.ts_piece(self.q, a)
                pltpu.make_async_copy(ref, ref, self.lsem.at[2]).wait()

    def ts_finish(self):
        @pl.when(self.r < 2)
        def _():
            dest = self.q % 8

            def one(i, carry):
                p = self.r * 16 + i

                @pl.when(jnp.logical_not((dest == self.r) & (p == self.q)))
                def _():
                    self.wait_send(self.ts_piece(0, 0), S_TS + i)

                return carry

            lax.fori_loop(0, 16, one, 0)

    def c_start(self):
        @pl.when(self.y == 0)
        def _():
            self.c_move(0)
            self.c_move(1)

    def c_pass(self, n):
        @pl.when(self.y != 0)
        def _():
            self.c_move(n)

    def c_move(self, n):
        far = self.y // 3
        h = far if n == 0 else 1 - far
        on = jnp.where(h == 0, self.y != 3, self.y != 1)
        row = (self.r + 2 + 4 * h) % 8

        def one(j, carry):
            i = h * 4 + j
            ref = self.chunk_c(self.k, i)

            @pl.when(self.y != 0)
            def _():
                self.wait_recv(ref, R_CR + i)

            @pl.when(on)
            def _():
                self.remote(ref, ref, S_CR + i, R_CR + i, self.coord(row=row)).start()

            self.remote(ref, ref, S_CS + i, R_CS + i, self.other).start()
            return carry

        lax.fori_loop(0, 4, one, 0)

    def c_finish(self):
        def one(i, carry):
            self.wait_recv(self.chunk_c(1 - self.k, i), R_CS + i)
            self.wait_send(self.chunk_c(self.k, i), S_CS + i)
            h = i // 4

            @pl.when(jnp.where(h == 0, self.y != 3, self.y != 1))
            def _():
                self.wait_send(self.chunk_c(self.k, i), S_CR + i)

            return carry

        lax.fori_loop(0, 8, one, 0)

    A_INFO = ((0, 0, R_A0, 16, 32, 0), (1, 0, R_A1, 8, 64, 16), (1, 1, R_A2, 8, 64, 24))

    def a_children(self, b):
        xs = self.A_INFO[b][0]
        z, y, x, r = self.z, self.y, self.x, self.r
        dx = (x - xs + 4) % 4
        z0 = z == 0
        zy0 = z0 & (y == 0)
        return (
            (z <= 3, self.coord(z=(z + 1) % 8)),
            (z0 | (z >= 6), self.coord(z=(z + 7) % 8)),
            (z0 & (y <= 1), self.coord(row=(r + 2) % 8)),
            (zy0, self.coord(row=(r + 6) % 8)),
            (zy0 & (dx <= 1), self.coord(x=(x + 1) % 4)),
            (zy0 & (dx == 0), self.coord(x=(x + 3) % 4)),
            (None, self.other),
        )

    def a_chunk(self, b, g, j):
        n = self.A_INFO[b][4]
        row = pl.multiple_of(g * 128 + j * n, n)
        lane = 0 if b == 1 else g * 128
        return self.a.at[b, pl.ds(row, n), lane:B]

    def a_loop(self, b, groups, fn):
        per = 128 // self.A_INFO[b][4]
        for g in groups:

            def one(j, carry):
                fn(self.a_chunk(b, g, j), g * per + j)
                return carry

            lax.fori_loop(0, per, one, 0)

    def a_relay(self, b, groups=range(4)):
        xs, ks, rs, s0 = self.A_INFO[b][:3] + self.A_INFO[b][5:]

        @pl.when(self.k == ks)
        def _():
            source = (self.z == 0) & (self.y == 0) & (self.x == xs)

            def one(ref, j):
                @pl.when(jnp.logical_not(source))
                def _():
                    self.wait_recv(ref, rs + j)

                for d, (cond, to) in enumerate(self.a_children(b)):
                    copy = self.remote(ref, ref, S_A + (s0 + j) * 7 + d, rs + j, to)
                    if cond is None:
                        copy.start()
                    else:
                        pl.when(cond)(copy.start)

            self.a_loop(b, groups, one)

    def a_take(self, b, groups=range(4)):
        ks, rs = self.A_INFO[b][1:3]

        @pl.when(self.k != ks)
        def _():
            self.a_loop(b, groups, lambda ref, j: self.wait_recv(ref, rs + j))

    def a_finish(self, blocks=range(3)):
        for b in blocks:
            ks, s0 = self.A_INFO[b][1], self.A_INFO[b][5]

            @pl.when(self.k == ks)
            def _():
                for d, (cond, _) in enumerate(self.a_children(b)):

                    def wait():
                        self.a_loop(b, range(4), lambda ref, j: self.wait_send(ref, S_A + (s0 + j) * 7 + d))

                    if cond is None:
                        wait()
                    else:
                        pl.when(cond)(wait)

    def shard(self, z, x, half):
        p = (z % 8) * 4 + x % 4
        if half == 0:
            return self.t.at[pl.ds(pl.multiple_of(p * 32, 8), ROW_SPLIT), :]
        return self.t.at[pl.ds(pl.multiple_of(p * 32 + ROW_SPLIT, 8), 32 - ROW_SPLIT), :]

    def zto(self, sign):
        return self.coord(z=(self.z + 8 + sign) % 8)

    def xto(self, sign):
        return self.coord(x=(self.x + 4 + sign) % 4)

    def p1z(self, op, sign, s):
        i = s if sign > 0 else 4 + s
        if op == "send":
            ref = self.shard(self.z + 8 - sign * s, self.x, 0)
            self.remote(ref, ref, S_P1Z + i, R_P1Z + i, self.zto(sign)).start()
        elif op == "recv":
            self.wait_recv(self.shard(self.z + 8 - sign * (s + 1), self.x, 0), R_P1Z + i)
        else:
            self.wait_send(self.shard(self.z, self.x, 0), S_P1Z + i)

    def p1x(self, op, sign, s):
        i = s if sign > 0 else 2 + s
        if op == "send":
            ref = self.shard(self.z, self.x + 4 - sign * s, 1)
            self.remote(ref, ref, S_P1X + i, R_P1X + i, self.xto(sign)).start()
        elif op == "recv":
            self.wait_recv(self.shard(self.z, self.x + 4 - sign * (s + 1), 1), R_P1X + i)
        else:
            self.wait_send(self.shard(self.z, self.x, 1), S_P1X + i)

    def p2x(self, op, sign, s, d):
        i = (0 if sign > 0 else 16) + s * 8 + d
        if op == "send":
            ref = self.shard(self.z + d, self.x + 4 - sign * s, 0)
            self.remote(ref, ref, S_P2X + i, R_P2X + i, self.xto(sign)).start()
        elif op == "recv":
            self.wait_recv(self.shard(self.z + d, self.x + 4 - sign * (s + 1), 0), R_P2X + i)
        else:
            self.wait_send(self.shard(self.z, self.x, 0), S_P2X + i)

    def p2z(self, op, sign, s, d):
        i = (0 if sign > 0 else 16) + s * 4 + d
        if op == "send":
            ref = self.shard(self.z + 8 - sign * s, self.x + d, 1)
            self.remote(ref, ref, S_P2Z + i, R_P2Z + i, self.zto(sign)).start()
        elif op == "recv":
            self.wait_recv(self.shard(self.z + 8 - sign * (s + 1), self.x + d, 1), R_P2Z + i)
        else:
            self.wait_send(self.shard(self.z, self.x, 1), S_P2Z + i)

    def p2z_pairs(self, s):
        if s < 3:
            return [(sign, d) for d in range(4) for sign in (1, -1)]
        return [(1, 0), (1, 1), (-1, 2), (-1, 3)]

    def t_stage(self, n):
        if n == 0:
            self.ts_wait()
            for sign in (1, -1):
                self.p1z("send", sign, 0)
                self.p1x("send", sign, 0)
        elif n == 1:
            for sign in (1, -1):
                self.p1z("recv", sign, 0)
                self.p1z("send", sign, 1)
                self.p1x("recv", sign, 0)
            self.p1x("send", 1, 1)
            for d in (0, 1, 7):
                for sign in (1, -1):
                    self.p2x("send", sign, 0, d)
        elif n == 2:
            for sign in (1, -1):
                self.p1z("recv", sign, 1)
                self.p1z("send", sign, 2)
            self.p1x("recv", 1, 1)
            for sign, d in self.p2z_pairs(0):
                self.p2z("send", sign, 0, d)
            for d in (2, 6):
                for sign in (1, -1):
                    self.p2x("send", sign, 0, d)
        elif n == 3:
            for sign in (1, -1):
                self.p1z("recv", sign, 2)
            self.p1z("send", 1, 3)
            for d in (3, 5):
                for sign in (1, -1):
                    self.p2x("send", sign, 0, d)
        elif n == 4:
            self.p1z("recv", 1, 3)
            for sign in (1, -1):
                self.p2x("send", sign, 0, 4)
            for sign, d in self.p2z_pairs(0):
                self.p2z("recv", sign, 0, d)
                self.p2z("send", sign, 1, d)
        elif n == 5:
            self.p2x_pass((0, 1, 7))
        elif n == 6:
            for sign, d in self.p2z_pairs(1):
                self.p2z("recv", sign, 1, d)
                self.p2z("send", sign, 2, d)
        elif n == 7:
            self.p2x_pass((2, 6))
        elif n == 8:
            last = self.p2z_pairs(3)
            for sign, d in self.p2z_pairs(2):
                self.p2z("recv", sign, 2, d)
                if (sign, d) in last:
                    self.p2z("send", sign, 3, d)
        elif n == 9:
            self.p2x_pass((3, 5, 4))
        elif n == 10:
            for d in Z_ORDER:
                self.p2x("recv", 1 if d % 2 == 0 else -1, 1, d)
            for sign, d in self.p2z_pairs(3):
                self.p2z("recv", sign, 3, d)

    def p2x_pass(self, ds):
        for d in ds:
            for sign in (1, -1):
                self.p2x("recv", sign, 0, d)
            self.p2x("send", 1 if d % 2 == 0 else -1, 1, d)

    def t_finish(self):
        self.ts_finish()
        for s in range(4):
            self.p1z("sent", 1, s)
        for s in range(3):
            self.p1z("sent", -1, s)
        self.p1x("sent", 1, 0)
        self.p1x("sent", 1, 1)
        self.p1x("sent", -1, 0)
        for d in range(8):
            self.p2x("sent", 1, 0, d)
            self.p2x("sent", -1, 0, d)
            self.p2x("sent", 1 if d % 2 == 0 else -1, 1, d)
        for s in range(4):
            for sign, d in self.p2z_pairs(s):
                self.p2z("sent", sign, s, d)


def dot(a, b):
    return jnp.dot(a, b, precision=HI, preferred_element_type=F32)


def dot_t(a, b):
    return lax.dot_general(a, b, (((0,), (0,)), ((), ())), precision=HI, preferred_element_type=F32)


def factor128(buf, ns, hook):
    width = buf.shape[1]
    rows = lax.broadcasted_iota(jnp.int32, (ns, 128), 0)
    for s in range(128 // ns):
        base = s * ns
        strip = [buf[base : base + ns, g * 128 : (g + 1) * 128] for g in range(width // 128)]
        cols = [jnp.broadcast_to(strip[0][:, base + j : base + j + 1], (ns, 128)) for j in range(ns)]
        for p in range(ns):
            r = lax.rsqrt(cols[p][p : p + 1, :])
            low = jnp.where(rows > p, cols[p], 0.0) * r
            for g in range(width // 128):
                u = strip[g][p : p + 1, :] * r
                buf[base + p : base + p + 1, g * 128 : (g + 1) * 128] = u
                strip[g] = strip[g] - low * u
            for j in range(p + 1, ns):
                cols[j] = cols[j] - low * (cols[j][p : p + 1, :] * r)
        nxt = base + ns
        if nxt < 128:
            u = buf[base:nxt, :]
            buf[nxt:128, :] = buf[nxt:128, :] - dot_t(u[:, nxt:128], u)
        hook(nxt)


def chol512(wk, buf, ns, hook):
    eye = (lax.broadcasted_iota(jnp.int32, (128, 128), 0) == lax.broadcasted_iota(jnp.int32, (128, 128), 1)).astype(F32)
    r5 = lax.broadcasted_iota(jnp.int32, (512, 512), 0)
    c5 = lax.broadcasted_iota(jnp.int32, (512, 512), 1)
    wk[:, 512:1024] = (r5 == c5).astype(F32)

    def step(kb, carry):
        off = pl.multiple_of(kb * 128, 128)
        buf[:, 0:128] = wk[pl.ds(off, 128), pl.ds(off, 128)]
        buf[:, 128:256] = eye
        factor128(buf, ns, functools.partial(hook, kb))
        new = dot(buf[:, 128:256], wk[pl.ds(off, 128), :])
        wk[pl.ds(off, 128), :] = new
        wk[pl.ds(off, 128), pl.ds(off, 128)] = buf[:, 0:128]

        def upd(j, c):
            o = pl.multiple_of(j * 128, 128)
            left = wk[pl.ds(off, 128), pl.ds(o, 128)]
            wk[pl.ds(o, 128), :] = wk[pl.ds(o, 128), :] - dot_t(left, wk[pl.ds(off, 128), :])
            return c

        lax.fori_loop(kb + 1, 4, upd, 0)
        return carry

    lax.fori_loop(0, 4, step, 0)


def fused_kernel(m_ref, t_ref, c_ref, w_ref, u_ref, a_ref, wk, buf, ssem, rsem, lsem):
    cm = Comm(m_ref, t_ref, c_ref, a_ref, ssem, rsem, lsem)
    cm.load()
    cm.barrier()
    cm.ts_send()
    cm.c_start()
    cm.a_relay(0)
    cm.a_take(0)

    def lead(g):
        cm.a_relay(1, (g,))
        cm.a_relay(2, (g,))

    def rest():
        cm.a_take(1)
        cm.a_take(2)

    plan = [
        (lambda: cm.t_stage(0),),
        (lambda: lead(0),),
        (lambda: cm.t_stage(1),),
        (lambda: lead(1),),
        (lambda: cm.t_stage(2), lambda: cm.c_pass(0)),
        (lambda: lead(2),),
        (lambda: cm.t_stage(3),),
        (lambda: lead(3), rest),
        (lambda: cm.t_stage(4), lambda: cm.c_pass(1)),
        (lambda: cm.t_stage(5),),
        (lambda: cm.t_stage(6),),
        (lambda: cm.t_stage(7),),
        (lambda: cm.t_stage(8),),
        (lambda: cm.t_stage(9),),
        (),
        (),
    ]
    upper = lax.broadcasted_iota(jnp.int32, (512, 512), 0) <= lax.broadcasted_iota(jnp.int32, (512, 512), 1)

    def half(h, c):
        @pl.when(h == 0)
        def _():
            wk[:, 0:512] = a_ref[0]

        @pl.when(h == 1)
        def _():
            u01 = dot(w_ref[0], a_ref[1])
            u_ref[2] = u01
            wk[:, 0:512] = a_ref[2] - dot_t(u01, u01)

        def hook(kb, done):
            if done % 64:
                return
            for i in range(8):
                acts = plan[2 * i + done // 64 - 1]
                if acts:

                    @pl.when(h * 4 + kb == i)
                    def _():
                        for act in acts:
                            act()

        chol512(wk, buf, NS, hook)
        u_ref[h] = jnp.where(upper, wk[:, 0:512], 0.0)
        w_ref[h] = wk[:, 512:1024]
        return c

    lax.fori_loop(0, 2, half, 0)
    cm.t_stage(10)
    cm.c_finish()
    cm.a_finish()
    cm.t_finish()


def fused(m):
    vm = pl.BlockSpec(memory_space=pltpu.VMEM)
    return pl.pallas_call(
        fused_kernel,
        out_shape=(
            jax.ShapeDtypeStruct((1024, 2048), F32),
            jax.ShapeDtypeStruct((1024, 512), F32),
            jax.ShapeDtypeStruct((2, 512, 512), F32),
            jax.ShapeDtypeStruct((3, 512, 512), F32),
        ),
        in_specs=[pl.BlockSpec(memory_space=pl.ANY)],
        out_specs=(vm,) * 4,
        scratch_shapes=[
            pltpu.VMEM((3, 512, 512), F32),
            pltpu.VMEM((512, 1024), F32),
            pltpu.VMEM((128, 256), F32),
            pltpu.SemaphoreType.DMA((N_SEND,)),
            pltpu.SemaphoreType.DMA((N_RECV,)),
            pltpu.SemaphoreType.DMA((3,)),
        ],
        compiler_params=pltpu.CompilerParams(
            collective_id=0, has_side_effects=True, vmem_limit_bytes=50 * 2**20
        ),
    )(m)


def split(v):
    hi = v.astype(BF16)
    return hi, (v - hi.astype(F32)).astype(BF16)


def dot3(a, b, dims):
    (ah, al), (bh, bl) = a, b
    d = functools.partial(lax.dot_general, dimension_numbers=(dims, ((), ())), preferred_element_type=F32)
    return d(al, bh) + d(ah, bl) + d(ah, bh)


NN = ((1,), (0,))
TN = ((0,), (0,))


def solve_pair(w0, w1, u01, top, bottom):
    x0 = dot3(w0, split(top), NN)
    x0s = split(x0)
    x1 = dot3(w1, split(bottom - dot3(u01, x0s, TN)), NN)
    return x0, x1, x0s, split(x1)


def update_kernel(f_ref, t_ref, c_ref, w_ref, u_ref, o_ref, wh, wl, yh, yl):
    a = pl.program_id(0)
    row = lax.axis_index("row")
    col = lax.axis_index("col") * 4 + lax.axis_index("depth")
    block = a * 8 + row

    @pl.when(a == 0)
    def _():
        for n, ref in enumerate((w_ref.at[0], w_ref.at[1], u_ref.at[2])):
            h, l = split(ref[...])
            wh[n] = h
            wl[n] = l

    w0, w1, u01 = ((wh[n], wl[n]) for n in range(3))

    @pl.when((a == 0) & (col >= 2))
    def _():
        _, _, y0, y1 = solve_pair(w0, w1, u01, c_ref[0:512, :], c_ref[512:1024, :])
        yh[0:512, :], yl[0:512, :] = y0
        yh[512:1024, :], yl[512:1024, :] = y1

    x0, x1, x0s, x1s = solve_pair(w0, w1, u01, t_ref[0:512, :], t_ref[512:1024, :])

    @pl.when(col == 0)
    def _():
        @pl.when(block == 0)
        def _():
            o_ref[0] = u_ref[0].T

        @pl.when(block != 0)
        def _():
            o_ref[0] = x0.T

    @pl.when(col == 1)
    def _():
        @pl.when(block == 0)
        def _():
            o_ref[0] = jnp.zeros((B, B), F32)

        @pl.when(block == 1)
        def _():
            o_ref[0] = u_ref[1].T

        @pl.when(block > 1)
        def _():
            o_ref[0] = x1.T

    @pl.when(col >= 2)
    def _():
        @pl.when(block <= 1)
        def _():
            o_ref[0] = jnp.zeros((B, B), F32)

        @pl.when(block > 1)
        def _():
            s = dot3(x0s, (yh[0:512, :], yl[0:512, :]), TN) + dot3(x1s, (yh[512:1024, :], yl[512:1024, :]), TN)
            o_ref[0] = f_ref[0] - s


def update(f, t, c, w, u):
    whole = lambda *shape: pl.BlockSpec(shape, lambda a: (0,) * len(shape))
    return pl.pallas_call(
        update_kernel,
        grid=(4,),
        out_shape=jax.ShapeDtypeStruct((4, B, B), F32),
        in_specs=[
            pl.BlockSpec((1, B, B), lambda a: (a, 0, 0)),
            pl.BlockSpec((1024, B), lambda a: (0, a)),
            whole(1024, 512),
            whole(2, B, B),
            whole(3, B, B),
        ],
        out_specs=pl.BlockSpec((1, B, B), lambda a: (a, 0, 0)),
        scratch_shapes=[
            pltpu.VMEM((3, B, B), BF16),
            pltpu.VMEM((3, B, B), BF16),
            pltpu.VMEM((1024, B), BF16),
            pltpu.VMEM((1024, B), BF16),
        ],
        compiler_params=pltpu.CompilerParams(
            dimension_semantics=("arbitrary",), vmem_limit_bytes=50 * 2**20
        ),
    )(f, t, c, w, u)


def body(matrix):
    t, c, w, u = fused(matrix)
    return update(matrix[:, 0], t, c, w, u)[:, None]


def solution(mesh):
    spec = P(None, "row", None, ("col", "depth"))
    return jax.shard_map(body, mesh=mesh, in_specs=(spec,), out_specs=spec, check_vma=False)
```

```python
import functools
import jax
import jax.numpy as jnp
from jax import lax
from jax.experimental import pallas as pl
from jax.experimental.pallas import tpu as pltpu
from jax.sharding import PartitionSpec as P

HI = lax.Precision.HIGHEST
F32 = jnp.float32
BF16 = jnp.bfloat16
MESH = pl.DeviceIdType.MESH
B = 512
ROW_SPLIT = 24
NS = 16
Z_ORDER = (0, 1, 7, 2, 6, 3, 5, 4)

R_TS = 0
R_CR = 4
R_CS = 12
R_A0 = 20
R_A1 = 36
R_A2 = 44
R_P1Z = 52
R_P1X = 60
R_P2X = 64
R_P2Z = 96
R_W = 128
N_RECV = 134
S_TS = 0
S_CR = 16
S_CS = 24
S_A = 32
S_P1Z = 256
S_P1X = 264
S_P2X = 268
S_P2Z = 300
S_W = 332
N_SEND = 338


class Comm:
    def __init__(self, m_ref, tbuf, cbuf, abuf, ssem, rsem, lsem):
        self.m, self.t, self.c, self.a = m_ref, tbuf, cbuf, abuf
        self.ssem, self.rsem, self.lsem = ssem, rsem, lsem
        self.r = lax.axis_index("row")
        self.z = lax.axis_index("col")
        self.x = lax.axis_index("depth")
        self.y = self.r // 2
        self.k = self.r % 2
        self.q = self.z * 4 + self.x
        self.other = self.coord(row=self.r + 1 - 2 * self.k)

    def coord(self, row=None, z=None, x=None):
        return {
            "row": self.r if row is None else row,
            "col": self.z if z is None else z,
            "depth": self.x if x is None else x,
        }

    def remote(self, src, dst, ssem, rsem, to):
        return pltpu.make_async_remote_copy(
            src_ref=src,
            dst_ref=dst,
            send_sem=self.ssem.at[ssem],
            recv_sem=self.rsem.at[rsem],
            device_id=to,
            device_id_type=MESH,
        )

    def wait_recv(self, ref, rsem):
        self.remote(ref, ref, 0, rsem, self.other).wait_recv()

    def wait_send(self, ref, ssem):
        self.remote(ref, ref, ssem, 0, self.other).wait_send()

    def barrier(self):
        sem = pltpu.get_barrier_semaphore()
        r, z, x, y, k, q = self.r, self.z, self.x, self.y, self.k, self.q
        ring = [
            self.coord(row=r + 1 - 2 * k),
            self.coord(row=(r + 2) % 8),
            self.coord(row=(r + 6) % 8),
            self.coord(z=(z + 1) % 8),
            self.coord(z=(z + 7) % 8),
            self.coord(x=(x + 1) % 4),
            self.coord(x=(x + 3) % 4),
        ]
        for to in ring:
            pl.semaphore_signal(sem, inc=1, device_id=to, device_id_type=MESH)
        mine = r == q // 16
        for a in range(4):
            col = 8 * a + r

            @pl.when(jnp.logical_not(mine & (col == q)))
            def _():
                to = self.coord(row=q // 16, z=col // 4, x=col % 4)
                pl.semaphore_signal(sem, inc=1, device_id=to, device_id_type=MESH)

        source = r < 2
        dest = q % 8

        @pl.when(source)
        def _():
            def one(i, carry):
                p = r * 16 + i

                @pl.when(jnp.logical_not((dest == r) & (p == q)))
                def _():
                    to = self.coord(row=dest, z=p // 4, x=p % 4)
                    pl.semaphore_signal(sem, inc=1, device_id=to, device_id_type=MESH)

                return carry

            lax.fori_loop(0, 16, one, 0)

        self.own = mine & (q % 8 == r)
        own = self.own.astype(jnp.int32)
        pl.semaphore_wait(sem, 11 - own + source.astype(jnp.int32) * (16 - own))

    def chunk_c(self, k, i):
        return self.c.at[pl.ds(pl.multiple_of(k * B + i * 64, 64), 64), :]

    def load(self):
        @pl.when(self.r < 2)
        def _():
            dst = self.c.at[pl.ds(pl.multiple_of(self.k * B, B), B), :]
            cp = pltpu.make_async_copy(self.m.at[0, 0], dst, self.lsem.at[0])
            cp.start()
            for b, (xs, ks) in enumerate(((0, 0), (0, 1), (1, 1))):

                @pl.when((self.z == 0) & (self.x == xs) & (self.k == ks))
                def _():
                    ca = pltpu.make_async_copy(self.m.at[0, 0], self.a.at[b], self.lsem.at[1])
                    ca.start()
                    ca.wait()

            cp.wait()

    def ts_piece(self, p, a):
        return self.t.at[pl.ds(pl.multiple_of(p * 32, 32), 32), pl.ds(pl.multiple_of(a * B, B), B)]

    def ts_send(self):
        @pl.when(self.r < 2)
        def _():
            dest = self.q % 8
            a = self.q // 8

            def one(i, carry):
                p = self.r * 16 + i
                src = self.c.at[pl.ds(pl.multiple_of(p * 32, 32), 32), :]
                dst = self.ts_piece(p, a)
                is_own = (dest == self.r) & (p == self.q)

                @pl.when(jnp.logical_not(is_own))
                def _():
                    to = self.coord(row=dest, z=p // 4, x=p % 4)
                    self.remote(src, dst, S_TS + i, R_TS + a, to).start()

                @pl.when(is_own)
                def _():
                    pltpu.make_async_copy(src, dst, self.lsem.at[2]).start()

                return carry

            lax.fori_loop(0, 16, one, 0)

    def ts_wait(self):
        for a in range(4):
            own = self.own & (self.q // 8 == a)

            @pl.when(jnp.logical_not(own))
            def _():
                self.wait_recv(self.ts_piece(self.q, a), R_TS + a)

            @pl.when(own)
            def _():
                ref = self.ts_piece(self.q, a)
                pltpu.make_async_copy(ref, ref, self.lsem.at[2]).wait()

    def ts_finish(self):
        @pl.when(self.r < 2)
        def _():
            dest = self.q % 8

            def one(i, carry):
                p = self.r * 16 + i

                @pl.when(jnp.logical_not((dest == self.r) & (p == self.q)))
                def _():
                    self.wait_send(self.ts_piece(0, 0), S_TS + i)

                return carry

            lax.fori_loop(0, 16, one, 0)

    def c_start(self):
        @pl.when(self.y == 0)
        def _():
            self.c_move(0)
            self.c_move(1)

    def c_pass(self, n):
        @pl.when(self.y % 2 == 1)
        def _():
            self.c_move(n)

        if n == 0:

            @pl.when(self.y == 2)
            def _():
                self.c_move(0)
                self.c_move(1)

    def c_move(self, n):
        far = self.y // 3
        h = far if n == 0 else 1 - far
        on = jnp.where(h == 0, self.y != 3, self.y != 1)
        row = (self.r + 2 + 4 * h) % 8

        def one(j, carry):
            i = h * 4 + j
            ref = self.chunk_c(self.k, i)

            @pl.when(self.y != 0)
            def _():
                self.wait_recv(ref, R_CR + i)

            @pl.when(on)
            def _():
                self.remote(ref, ref, S_CR + i, R_CR + i, self.coord(row=row)).start()

            self.remote(ref, ref, S_CS + i, R_CS + i, self.other).start()
            return carry

        lax.fori_loop(0, 4, one, 0)

    def c_finish(self):
        def one(i, carry):
            self.wait_recv(self.chunk_c(1 - self.k, i), R_CS + i)
            self.wait_send(self.chunk_c(self.k, i), S_CS + i)
            h = i // 4

            @pl.when(jnp.where(h == 0, self.y != 3, self.y != 1))
            def _():
                self.wait_send(self.chunk_c(self.k, i), S_CR + i)

            return carry

        lax.fori_loop(0, 8, one, 0)

    A_INFO = ((0, 0, R_A0, 16, 32, 0), (0, 1, R_A1, 8, 64, 16), (1, 1, R_A2, 8, 64, 24))

    def a_children(self, b):
        xs = self.A_INFO[b][0]
        z, y, x, r = self.z, self.y, self.x, self.r
        dx = (x - xs + 4) % 4
        z0, y0 = z == 0, y == 0
        on_x = y0 if b == 1 else y0 & z0
        on_z = y0 & (dx == 0) if b == 1 else z >= 0
        on_y = z >= 0 if b == 1 else z0
        return (
            (on_z & (z <= 3), self.coord(z=(z + 1) % 8)),
            (on_z & (z0 | (z >= 6)), self.coord(z=(z + 7) % 8)),
            (on_y & (y <= 1), self.coord(row=(r + 2) % 8)),
            (on_y & y0, self.coord(row=(r + 6) % 8)),
            (on_x & (dx <= 1), self.coord(x=(x + 1) % 4)),
            (on_x & (dx == 0), self.coord(x=(x + 3) % 4)),
        ) + (((None, self.other),) if b else ())

    def a_chunk(self, b, g, j):
        n = self.A_INFO[b][4]
        row = pl.multiple_of(g * 128 + j * n, n)
        lane = 0 if b == 1 else g * 128
        return self.a.at[b, pl.ds(row, n), lane:B]

    def a_loop(self, b, groups, fn):
        per = 128 // self.A_INFO[b][4]
        for g in groups:

            def one(j, carry):
                fn(self.a_chunk(b, g, j), g * per + j)
                return carry

            lax.fori_loop(0, per, one, 0)

    def a_relay(self, b, groups=range(4)):
        xs, ks, rs, s0 = self.A_INFO[b][:3] + self.A_INFO[b][5:]

        @pl.when(self.k == ks)
        def _():
            source = (self.z == 0) & (self.y == 0) & (self.x == xs)

            def one(ref, j):
                @pl.when(jnp.logical_not(source))
                def _():
                    self.wait_recv(ref, rs + j)

                for d, (cond, to) in enumerate(self.a_children(b)):
                    copy = self.remote(ref, ref, S_A + (s0 + j) * 7 + d, rs + j, to)
                    if cond is None:
                        copy.start()
                    else:
                        pl.when(cond)(copy.start)

            self.a_loop(b, groups, one)

    def a_take(self, b, groups=range(4)):
        ks, rs = self.A_INFO[b][1:3]

        @pl.when(self.k != ks)
        def _():
            self.a_loop(b, groups, lambda ref, j: self.wait_recv(ref, rs + j))

    def a_finish(self, blocks=range(3)):
        for b in blocks:
            ks, s0 = self.A_INFO[b][1], self.A_INFO[b][5]

            @pl.when(self.k == ks)
            def _():
                def one(ref, j):
                    for d, (cond, _) in enumerate(self.a_children(b)):
                        copy = self.remote(ref, ref, S_A + (s0 + j) * 7 + d, 0, self.other)
                        if cond is None:
                            copy.wait_send()
                        else:
                            pl.when(cond)(copy.wait_send)

                self.a_loop(b, range(4), one)

    def factors(self, w, u, z):
        return (w.at[0], w.at[1], u.at[0], u.at[1], u.at[2], z)

    def give(self, refs, n):
        self.remote(refs[n], refs[n], S_W + n, R_W + n, self.other).start()

    def shard(self, z, x, half):
        p = (z % 8) * 4 + x % 4
        if half == 0:
            return self.t.at[pl.ds(pl.multiple_of(p * 32, 8), ROW_SPLIT), :]
        return self.t.at[pl.ds(pl.multiple_of(p * 32 + ROW_SPLIT, 8), 32 - ROW_SPLIT), :]

    def zto(self, sign):
        return self.coord(z=(self.z + 8 + sign) % 8)

    def xto(self, sign):
        return self.coord(x=(self.x + 4 + sign) % 4)

    def p1z(self, op, sign, s):
        i = s if sign > 0 else 4 + s
        if op == "send":
            ref = self.shard(self.z + 8 - sign * s, self.x, 0)
            self.remote(ref, ref, S_P1Z + i, R_P1Z + i, self.zto(sign)).start()
        elif op == "recv":
            self.wait_recv(self.shard(self.z + 8 - sign * (s + 1), self.x, 0), R_P1Z + i)
        else:
            self.wait_send(self.shard(self.z, self.x, 0), S_P1Z + i)

    def p1x(self, op, sign, s):
        i = s if sign > 0 else 2 + s
        if op == "send":
            ref = self.shard(self.z, self.x + 4 - sign * s, 1)
            self.remote(ref, ref, S_P1X + i, R_P1X + i, self.xto(sign)).start()
        elif op == "recv":
            self.wait_recv(self.shard(self.z, self.x + 4 - sign * (s + 1), 1), R_P1X + i)
        else:
            self.wait_send(self.shard(self.z, self.x, 1), S_P1X + i)

    def p2x(self, op, sign, s, d):
        i = (0 if sign > 0 else 16) + s * 8 + d
        if op == "send":
            ref = self.shard(self.z + d, self.x + 4 - sign * s, 0)
            self.remote(ref, ref, S_P2X + i, R_P2X + i, self.xto(sign)).start()
        elif op == "recv":
            self.wait_recv(self.shard(self.z + d, self.x + 4 - sign * (s + 1), 0), R_P2X + i)
        else:
            self.wait_send(self.shard(self.z, self.x, 0), S_P2X + i)

    def p2z(self, op, sign, s, d):
        i = (0 if sign > 0 else 16) + s * 4 + d
        if op == "send":
            ref = self.shard(self.z + 8 - sign * s, self.x + d, 1)
            self.remote(ref, ref, S_P2Z + i, R_P2Z + i, self.zto(sign)).start()
        elif op == "recv":
            self.wait_recv(self.shard(self.z + 8 - sign * (s + 1), self.x + d, 1), R_P2Z + i)
        else:
            self.wait_send(self.shard(self.z, self.x, 1), S_P2Z + i)

    def p2z_pairs(self, s):
        if s < 3:
            return [(sign, d) for d in range(4) for sign in (1, -1)]
        return [(1, 0), (1, 1), (-1, 2), (-1, 3)]

    def t_stage(self, n):
        if n == 0:
            self.ts_wait()
            for sign in (1, -1):
                self.p1z("send", sign, 0)
                self.p1x("send", sign, 0)
        elif n == 1:
            for sign in (1, -1):
                self.p1z("recv", sign, 0)
                self.p1z("send", sign, 1)
                self.p1x("recv", sign, 0)
            self.p1x("send", 1, 1)
            for d in (0, 1, 7):
                for sign in (1, -1):
                    self.p2x("send", sign, 0, d)
        elif n == 2:
            for sign in (1, -1):
                self.p1z("recv", sign, 1)
                self.p1z("send", sign, 2)
            self.p1x("recv", 1, 1)
            for sign, d in self.p2z_pairs(0):
                self.p2z("send", sign, 0, d)
            for d in (2, 6):
                for sign in (1, -1):
                    self.p2x("send", sign, 0, d)
        elif n == 3:
            for sign in (1, -1):
                self.p1z("recv", sign, 2)
            self.p1z("send", 1, 3)
            for d in (3, 5):
                for sign in (1, -1):
                    self.p2x("send", sign, 0, d)
        elif n == 4:
            self.p1z("recv", 1, 3)
            for sign in (1, -1):
                self.p2x("send", sign, 0, 4)
            for sign, d in self.p2z_pairs(0):
                self.p2z("recv", sign, 0, d)
                self.p2z("send", sign, 1, d)
        elif n == 5:
            self.p2x_pass((0, 1, 7))
        elif n == 6:
            for sign, d in self.p2z_pairs(1):
                self.p2z("recv", sign, 1, d)
                self.p2z("send", sign, 2, d)
        elif n == 7:
            self.p2x_pass((2, 6))
        elif n == 8:
            last = self.p2z_pairs(3)
            for sign, d in self.p2z_pairs(2):
                self.p2z("recv", sign, 2, d)
                if (sign, d) in last:
                    self.p2z("send", sign, 3, d)
        elif n == 9:
            self.p2x_pass((3, 5, 4))
        elif n == 10:
            for d in Z_ORDER:
                self.p2x("recv", 1 if d % 2 == 0 else -1, 1, d)
            for sign, d in self.p2z_pairs(3):
                self.p2z("recv", sign, 3, d)

    def p2x_pass(self, ds):
        for d in ds:
            for sign in (1, -1):
                self.p2x("recv", sign, 0, d)
            self.p2x("send", 1 if d % 2 == 0 else -1, 1, d)

    def t_finish(self):
        self.ts_finish()
        for s in range(4):
            self.p1z("sent", 1, s)
        for s in range(3):
            self.p1z("sent", -1, s)
        self.p1x("sent", 1, 0)
        self.p1x("sent", 1, 1)
        self.p1x("sent", -1, 0)
        for d in range(8):
            self.p2x("sent", 1, 0, d)
            self.p2x("sent", -1, 0, d)
            self.p2x("sent", 1 if d % 2 == 0 else -1, 1, d)
        for s in range(4):
            for sign, d in self.p2z_pairs(s):
                self.p2z("sent", sign, s, d)


def dot(a, b):
    return jnp.dot(a, b, precision=HI, preferred_element_type=F32)


def dot_t(a, b):
    return lax.dot_general(a, b, (((0,), (0,)), ((), ())), precision=HI, preferred_element_type=F32)


def factor128(buf, ns, hook):
    width = buf.shape[1]
    rows = lax.broadcasted_iota(jnp.int32, (ns, 128), 0)
    for s in range(128 // ns):
        base = s * ns
        strip = [buf[base : base + ns, g * 128 : (g + 1) * 128] for g in range(width // 128)]
        cols = [jnp.broadcast_to(strip[0][:, base + j : base + j + 1], (ns, 128)) for j in range(ns)]
        for p in range(ns):
            r = lax.rsqrt(cols[p][p : p + 1, :])
            low = jnp.where(rows > p, cols[p], 0.0) * r
            for g in range(width // 128):
                u = strip[g][p : p + 1, :] * r
                buf[base + p : base + p + 1, g * 128 : (g + 1) * 128] = u
                strip[g] = strip[g] - low * u
            for j in range(p + 1, ns):
                cols[j] = cols[j] - low * (cols[j][p : p + 1, :] * r)
        nxt = base + ns
        if nxt < 128:
            u = buf[base:nxt, :]
            buf[nxt:128, :] = buf[nxt:128, :] - dot_t(u[:, nxt:128], u)
        hook(nxt)


def chol512(wk, buf, ns, hook):
    eye = (lax.broadcasted_iota(jnp.int32, (128, 128), 0) == lax.broadcasted_iota(jnp.int32, (128, 128), 1)).astype(F32)
    r5 = lax.broadcasted_iota(jnp.int32, (512, 512), 0)
    c5 = lax.broadcasted_iota(jnp.int32, (512, 512), 1)
    wk[:, 512:1024] = (r5 == c5).astype(F32)

    def step(kb, carry):
        off = pl.multiple_of(kb * 128, 128)
        buf[:, 0:128] = wk[pl.ds(off, 128), pl.ds(off, 128)]
        buf[:, 128:256] = eye
        factor128(buf, ns, functools.partial(hook, kb))
        new = dot(buf[:, 128:256], wk[pl.ds(off, 128), :])
        wk[pl.ds(off, 128), :] = new
        wk[pl.ds(off, 128), pl.ds(off, 128)] = buf[:, 0:128]

        def upd(j, c):
            o = pl.multiple_of(j * 128, 128)
            left = wk[pl.ds(off, 128), pl.ds(o, 128)]
            wk[pl.ds(o, 128), :] = wk[pl.ds(o, 128), :] - dot_t(left, wk[pl.ds(off, 128), :])
            return c

        lax.fori_loop(kb + 1, 4, upd, 0)
        return carry

    lax.fori_loop(0, 4, step, 0)


def column_solve(c_ref, w_ref, u_ref, z_ref):
    def chunk(n, carry):
        lanes = pl.ds(pl.multiple_of(n * 256, 256), 256)
        y0 = dot(w_ref[0], c_ref[0:512, lanes])
        y1 = dot(w_ref[1], c_ref[512:1024, lanes] - dot_t(u_ref[2], y0))
        z1 = dot_t(w_ref[1], y1)
        z0 = dot_t(w_ref[0], y0 - dot(u_ref[2], z1))
        z_ref[0:512, lanes] = z0
        z_ref[512:1024, lanes] = z1
        return carry

    lax.fori_loop(0, 2, chunk, 0)


def fused_kernel(m_ref, t_ref, zh_ref, zl_ref, w_ref, u_ref, c_ref, a_ref, z_ref, wk, buf, ssem, rsem, lsem):
    cm = Comm(m_ref, t_ref, c_ref, a_ref, ssem, rsem, lsem)
    refs = cm.factors(w_ref, u_ref, z_ref)
    cm.load()
    cm.barrier()
    cm.ts_send()
    cm.c_start()

    @pl.when(cm.k == 1)
    def _():
        cm.a_relay(1)
        cm.a_relay(2)
        for n in range(11):
            cm.t_stage(n)
            if n in (2, 5):
                cm.c_pass(n // 4)
        cm.c_finish()
        for n, ref in enumerate(refs):
            cm.wait_recv(ref, R_W + n)

    @pl.when(cm.k == 0)
    def _():
        cm.a_relay(0)
        factor(cm, refs, a_ref, w_ref, u_ref, wk, buf)
        cm.c_finish()
        column_solve(c_ref, w_ref, u_ref, z_ref)
        cm.t_stage(10)
        cm.give(refs, 5)
        for n, ref in enumerate(refs):
            cm.wait_send(ref, S_W + n)

    zh_ref[...], zl_ref[...] = split(z_ref[...])
    cm.a_finish()
    cm.t_finish()


def factor(cm, refs, a_ref, w_ref, u_ref, wk, buf):
    def rest():
        cm.a_take(1)
        cm.a_take(2)

    T = lambda n: (functools.partial(cm.t_stage, n),)
    C = lambda n: (functools.partial(cm.c_pass, n),)
    R = (rest,)
    plan = [
        T(0),
        T(1),
        T(2),
        T(3),
        C(0) + T(4),
        (),
        T(5),
        R,
        T(6) + C(1),
        T(7),
        (),
        T(8),
        (),
        T(9),
        (),
        (),
    ]
    upper = lax.broadcasted_iota(jnp.int32, (512, 512), 0) <= lax.broadcasted_iota(jnp.int32, (512, 512), 1)

    def half(h, c):
        @pl.when(h == 0)
        def _():
            wk[:, 0:512] = a_ref[0]

        @pl.when(h == 1)
        def _():
            u01 = lax.dot_general(w_ref[0], a_ref[1], (((1,), (1,)), ((), ())), precision=HI, preferred_element_type=F32)
            u_ref[2] = u01
            wk[:, 0:512] = a_ref[2] - dot_t(u01, u01)

        def hook(kb, done):
            if done % 64:
                return
            for i in range(8):
                acts = plan[2 * i + done // 64 - 1]
                if acts:

                    @pl.when(h * 4 + kb == i)
                    def _():
                        for act in acts:
                            act()

        chol512(wk, buf, NS, hook)
        u_ref[h] = jnp.where(upper, wk[:, 0:512], 0.0)
        w_ref[h] = wk[:, 512:1024]
        return c

    lax.fori_loop(0, 2, half, 0)
    for n in range(5):
        cm.give(refs, n)


def fused(m):
    vm = pl.BlockSpec(memory_space=pltpu.VMEM)
    return pl.pallas_call(
        fused_kernel,
        out_shape=(
            jax.ShapeDtypeStruct((1024, 2048), F32),
            jax.ShapeDtypeStruct((1024, 512), BF16),
            jax.ShapeDtypeStruct((1024, 512), BF16),
            jax.ShapeDtypeStruct((2, 512, 512), F32),
            jax.ShapeDtypeStruct((3, 512, 512), F32),
        ),
        in_specs=[pl.BlockSpec(memory_space=pl.ANY)],
        out_specs=(vm,) * 5,
        scratch_shapes=[
            pltpu.VMEM((1024, 512), F32),
            pltpu.VMEM((3, 512, 512), F32),
            pltpu.VMEM((1024, 512), F32),
            pltpu.VMEM((512, 1024), F32),
            pltpu.VMEM((128, 256), F32),
            pltpu.SemaphoreType.DMA((N_SEND,)),
            pltpu.SemaphoreType.DMA((N_RECV,)),
            pltpu.SemaphoreType.DMA((3,)),
        ],
        compiler_params=pltpu.CompilerParams(
            collective_id=0, has_side_effects=True, vmem_limit_bytes=50 * 2**20
        ),
    )(m)


def split(v):
    hi = v.astype(BF16)
    return hi, (v - hi.astype(F32)).astype(BF16)


def dot3(a, b, dims):
    (ah, al), (bh, bl) = a, b
    d = functools.partial(lax.dot_general, dimension_numbers=(dims, ((), ())), preferred_element_type=F32)
    return d(al, bh) + d(ah, bl) + d(ah, bh)


NN = ((1,), (0,))
TN = ((0,), (0,))


def update_kernel(f_ref, t_ref, zh_ref, zl_ref, w_ref, u_ref, o_ref):
    a = pl.program_id(0)
    row = lax.axis_index("row")
    col = lax.axis_index("col") * 4 + lax.axis_index("depth")
    block = a * 8 + row

    def x0():
        return dot3(split(w_ref[0]), split(t_ref[0:512, :]), NN)

    @pl.when((col >= 2) & (block > 1))
    def _():
        o_ref[0] = f_ref[0] - dot3(split(t_ref[...]), (zh_ref[...], zl_ref[...]), TN)

    @pl.when(block < jnp.minimum(col, 2))
    def _():
        o_ref[0] = jnp.zeros((B, B), F32)

    @pl.when((block == col) & (col < 2))
    def _():
        o_ref[0] = u_ref[jnp.minimum(col, 1)].T

    @pl.when((col == 0) & (block > 0))
    def _():
        o_ref[0] = x0().T

    @pl.when((col == 1) & (block > 1))
    def _():
        rest = t_ref[512:1024, :] - dot3(split(u_ref[2]), split(x0()), TN)
        o_ref[0] = dot3(split(w_ref[1]), split(rest), NN).T


def update(f, t, zh, zl, w, u):
    whole = lambda *shape: pl.BlockSpec(shape, lambda a: (0,) * len(shape))
    return pl.pallas_call(
        update_kernel,
        grid=(4,),
        out_shape=jax.ShapeDtypeStruct((4, B, B), F32),
        in_specs=[
            pl.BlockSpec((1, B, B), lambda a: (a, 0, 0)),
            pl.BlockSpec((1024, B), lambda a: (0, a)),
            whole(1024, B),
            whole(1024, B),
            whole(2, B, B),
            whole(3, B, B),
        ],
        out_specs=pl.BlockSpec((1, B, B), lambda a: (a, 0, 0)),
        compiler_params=pltpu.CompilerParams(
            dimension_semantics=("arbitrary",), vmem_limit_bytes=50 * 2**20
        ),
    )(f, t, zh, zl, w, u)


def body(matrix):
    return update(matrix[:, 0], *fused(matrix))[:, None]


def solution(mesh):
    spec = P(None, "row", None, ("col", "depth"))
    return jax.shard_map(body, mesh=mesh, in_specs=(spec,), out_specs=spec, check_vma=False)
```

```python
import functools
import jax
import jax.numpy as jnp
from jax import lax
from jax.experimental import pallas as pl
from jax.experimental.pallas import tpu as pltpu
from jax.sharding import PartitionSpec as P

HI = lax.Precision.HIGHEST
F32 = jnp.float32
BF16 = jnp.bfloat16
MESH = pl.DeviceIdType.MESH
B = 512
ROW_SPLIT = 24
NS = 16
Z_ORDER = (0, 1, 7, 2, 6, 3, 5, 4)

R_TS = 0
R_CR = 4
R_CS = 12
R_A0 = 20
R_A1 = 36
R_A2 = 44
R_P1Z = 52
R_P1X = 60
R_P2X = 64
R_P2Z = 96
R_W = 128
N_RECV = 134
S_TS = 0
S_CR = 16
S_CS = 24
S_A = 32
S_P1Z = 256
S_P1X = 264
S_P2X = 268
S_P2Z = 300
S_W = 332
N_SEND = 338


class Comm:
    def __init__(self, m_ref, tbuf, cbuf, abuf, ssem, rsem, lsem):
        self.m, self.t, self.c, self.a = m_ref, tbuf, cbuf, abuf
        self.ssem, self.rsem, self.lsem = ssem, rsem, lsem
        self.r = lax.axis_index("row")
        self.z = lax.axis_index("col")
        self.x = lax.axis_index("depth")
        self.y = self.r // 2
        self.k = self.r % 2
        self.q = self.z * 4 + self.x
        self.other = self.coord(row=self.r + 1 - 2 * self.k)

    def coord(self, row=None, z=None, x=None):
        return {
            "row": self.r if row is None else row,
            "col": self.z if z is None else z,
            "depth": self.x if x is None else x,
        }

    def remote(self, src, dst, ssem, rsem, to):
        return pltpu.make_async_remote_copy(
            src_ref=src,
            dst_ref=dst,
            send_sem=self.ssem.at[ssem],
            recv_sem=self.rsem.at[rsem],
            device_id=to,
            device_id_type=MESH,
        )

    def wait_recv(self, ref, rsem):
        self.remote(ref, ref, 0, rsem, self.other).wait_recv()

    def wait_send(self, ref, ssem):
        self.remote(ref, ref, ssem, 0, self.other).wait_send()

    def barrier(self):
        sem = pltpu.get_barrier_semaphore()
        r, z, x, y, k, q = self.r, self.z, self.x, self.y, self.k, self.q
        ring = [
            self.coord(row=r + 1 - 2 * k),
            self.coord(row=(r + 2) % 8),
            self.coord(row=(r + 6) % 8),
            self.coord(z=(z + 1) % 8),
            self.coord(z=(z + 7) % 8),
            self.coord(x=(x + 1) % 4),
            self.coord(x=(x + 3) % 4),
        ]
        for to in ring:
            pl.semaphore_signal(sem, inc=1, device_id=to, device_id_type=MESH)
        mine = r == q // 16
        for a in range(4):
            col = 8 * a + r

            @pl.when(jnp.logical_not(mine & (col == q)))
            def _():
                to = self.coord(row=q // 16, z=col // 4, x=col % 4)
                pl.semaphore_signal(sem, inc=1, device_id=to, device_id_type=MESH)

        source = r < 2
        dest = q % 8

        @pl.when(source)
        def _():
            def one(i, carry):
                p = r * 16 + i

                @pl.when(jnp.logical_not((dest == r) & (p == q)))
                def _():
                    to = self.coord(row=dest, z=p // 4, x=p % 4)
                    pl.semaphore_signal(sem, inc=1, device_id=to, device_id_type=MESH)

                return carry

            lax.fori_loop(0, 16, one, 0)

        self.own = mine & (q % 8 == r)
        own = self.own.astype(jnp.int32)
        pl.semaphore_wait(sem, 11 - own + source.astype(jnp.int32) * (16 - own))

    def chunk_c(self, k, i):
        return self.c.at[pl.ds(pl.multiple_of(k * B + i * 64, 64), 64), :]

    def load(self):
        @pl.when(self.r < 2)
        def _():
            dst = self.c.at[pl.ds(pl.multiple_of(self.k * B, B), B), :]
            cp = pltpu.make_async_copy(self.m.at[0, 0], dst, self.lsem.at[0])
            cp.start()
            for b, (xs, ks) in enumerate(((0, 0), (0, 1), (1, 1))):

                @pl.when((self.z == 0) & (self.x == xs) & (self.k == ks))
                def _():
                    ca = pltpu.make_async_copy(self.m.at[0, 0], self.a.at[b], self.lsem.at[1])
                    ca.start()
                    ca.wait()

            cp.wait()

    def ts_piece(self, p, a):
        return self.t.at[pl.ds(pl.multiple_of(p * 32, 32), 32), pl.ds(pl.multiple_of(a * B, B), B)]

    def ts_send(self):
        @pl.when(self.r < 2)
        def _():
            dest = self.q % 8
            a = self.q // 8

            def one(i, carry):
                p = self.r * 16 + i
                src = self.c.at[pl.ds(pl.multiple_of(p * 32, 32), 32), :]
                dst = self.ts_piece(p, a)
                is_own = (dest == self.r) & (p == self.q)

                @pl.when(jnp.logical_not(is_own))
                def _():
                    to = self.coord(row=dest, z=p // 4, x=p % 4)
                    self.remote(src, dst, S_TS + i, R_TS + a, to).start()

                @pl.when(is_own)
                def _():
                    pltpu.make_async_copy(src, dst, self.lsem.at[2]).start()

                return carry

            lax.fori_loop(0, 16, one, 0)

    def ts_wait(self):
        for a in range(4):
            own = self.own & (self.q // 8 == a)

            @pl.when(jnp.logical_not(own))
            def _():
                self.wait_recv(self.ts_piece(self.q, a), R_TS + a)

            @pl.when(own)
            def _():
                ref = self.ts_piece(self.q, a)
                pltpu.make_async_copy(ref, ref, self.lsem.at[2]).wait()

    def ts_finish(self):
        @pl.when(self.r < 2)
        def _():
            dest = self.q % 8

            def one(i, carry):
                p = self.r * 16 + i

                @pl.when(jnp.logical_not((dest == self.r) & (p == self.q)))
                def _():
                    self.wait_send(self.ts_piece(0, 0), S_TS + i)

                return carry

            lax.fori_loop(0, 16, one, 0)

    def c_start(self):
        @pl.when(self.y == 0)
        def _():
            self.c_move(0)
            self.c_move(1)

    def c_pass(self, n):
        @pl.when(self.y % 2 == 1)
        def _():
            self.c_move(n)

        if n == 0:

            @pl.when(self.y == 2)
            def _():
                self.c_move(0)
                self.c_move(1)

    def c_move(self, n):
        far = self.y // 3
        h = far if n == 0 else 1 - far
        on = jnp.where(h == 0, self.y != 3, self.y != 1)
        row = (self.r + 2 + 4 * h) % 8

        def one(j, carry):
            i = h * 4 + j
            ref = self.chunk_c(self.k, i)

            @pl.when(self.y != 0)
            def _():
                self.wait_recv(ref, R_CR + i)

            @pl.when(on)
            def _():
                self.remote(ref, ref, S_CR + i, R_CR + i, self.coord(row=row)).start()

            self.remote(ref, ref, S_CS + i, R_CS + i, self.other).start()
            return carry

        lax.fori_loop(0, 4, one, 0)

    def c_finish(self):
        def one(i, carry):
            self.wait_recv(self.chunk_c(1 - self.k, i), R_CS + i)
            self.wait_send(self.chunk_c(self.k, i), S_CS + i)
            h = i // 4

            @pl.when(jnp.where(h == 0, self.y != 3, self.y != 1))
            def _():
                self.wait_send(self.chunk_c(self.k, i), S_CR + i)

            return carry

        lax.fori_loop(0, 8, one, 0)

    A_INFO = ((0, 0, R_A0, 16, 32, 0), (0, 1, R_A1, 8, 64, 16), (1, 1, R_A2, 8, 64, 24))

    def a_children(self, b):
        xs = self.A_INFO[b][0]
        z, y, x, r = self.z, self.y, self.x, self.r
        dx = (x - xs + 4) % 4
        z0, y0 = z == 0, y == 0
        on_x = y0 if b == 1 else y0 & z0
        on_z = y0 & (dx == 0) if b == 1 else z >= 0
        on_y = z >= 0 if b == 1 else z0
        return (
            (on_z & (z <= 3), self.coord(z=(z + 1) % 8)),
            (on_z & (z0 | (z >= 6)), self.coord(z=(z + 7) % 8)),
            (on_y & (y <= 1), self.coord(row=(r + 2) % 8)),
            (on_y & y0, self.coord(row=(r + 6) % 8)),
            (on_x & (dx <= 1), self.coord(x=(x + 1) % 4)),
            (on_x & (dx == 0), self.coord(x=(x + 3) % 4)),
        ) + (((None, self.other),) if b else ())

    def a_chunk(self, b, g, j):
        n = self.A_INFO[b][4]
        row = pl.multiple_of(g * 128 + j * n, n)
        lane = 0 if b == 1 else g * 128
        return self.a.at[b, pl.ds(row, n), lane:B]

    def a_loop(self, b, groups, fn):
        per = 128 // self.A_INFO[b][4]
        for g in groups:

            def one(j, carry):
                fn(self.a_chunk(b, g, j), g * per + j)
                return carry

            lax.fori_loop(0, per, one, 0)

    def a_relay(self, b, groups=range(4)):
        xs, ks, rs, s0 = self.A_INFO[b][:3] + self.A_INFO[b][5:]

        @pl.when(self.k == ks)
        def _():
            source = (self.z == 0) & (self.y == 0) & (self.x == xs)

            def one(ref, j):
                @pl.when(jnp.logical_not(source))
                def _():
                    self.wait_recv(ref, rs + j)

                for d, (cond, to) in enumerate(self.a_children(b)):
                    copy = self.remote(ref, ref, S_A + (s0 + j) * 7 + d, rs + j, to)
                    if cond is None:
                        copy.start()
                    else:
                        pl.when(cond)(copy.start)

            self.a_loop(b, groups, one)

    def a_take(self, b, groups=range(4)):
        ks, rs = self.A_INFO[b][1:3]

        @pl.when(self.k != ks)
        def _():
            self.a_loop(b, groups, lambda ref, j: self.wait_recv(ref, rs + j))

    def a_finish(self, blocks=range(3)):
        for b in blocks:
            ks, s0 = self.A_INFO[b][1], self.A_INFO[b][5]

            @pl.when(self.k == ks)
            def _():
                def one(ref, j):
                    for d, (cond, _) in enumerate(self.a_children(b)):
                        copy = self.remote(ref, ref, S_A + (s0 + j) * 7 + d, 0, self.other)
                        if cond is None:
                            copy.wait_send()
                        else:
                            pl.when(cond)(copy.wait_send)

                self.a_loop(b, range(4), one)

    def factors(self, w, u):
        return (w.at[0], w.at[1], u.at[2], u.at[1])

    def give(self, refs, n):
        self.remote(refs[n], refs[n], S_W + n, R_W + n, self.other).start()

    def shard(self, z, x, half):
        p = (z % 8) * 4 + x % 4
        if half == 0:
            return self.t.at[pl.ds(pl.multiple_of(p * 32, 8), ROW_SPLIT), :]
        return self.t.at[pl.ds(pl.multiple_of(p * 32 + ROW_SPLIT, 8), 32 - ROW_SPLIT), :]

    def zto(self, sign):
        return self.coord(z=(self.z + 8 + sign) % 8)

    def xto(self, sign):
        return self.coord(x=(self.x + 4 + sign) % 4)

    def p1z(self, op, sign, s):
        i = s if sign > 0 else 4 + s
        if op == "send":
            ref = self.shard(self.z + 8 - sign * s, self.x, 0)
            self.remote(ref, ref, S_P1Z + i, R_P1Z + i, self.zto(sign)).start()
        elif op == "recv":
            self.wait_recv(self.shard(self.z + 8 - sign * (s + 1), self.x, 0), R_P1Z + i)
        else:
            self.wait_send(self.shard(self.z, self.x, 0), S_P1Z + i)

    def p1x(self, op, sign, s):
        i = s if sign > 0 else 2 + s
        if op == "send":
            ref = self.shard(self.z, self.x + 4 - sign * s, 1)
            self.remote(ref, ref, S_P1X + i, R_P1X + i, self.xto(sign)).start()
        elif op == "recv":
            self.wait_recv(self.shard(self.z, self.x + 4 - sign * (s + 1), 1), R_P1X + i)
        else:
            self.wait_send(self.shard(self.z, self.x, 1), S_P1X + i)

    def p2x(self, op, sign, s, d):
        i = (0 if sign > 0 else 16) + s * 8 + d
        if op == "send":
            ref = self.shard(self.z + d, self.x + 4 - sign * s, 0)
            self.remote(ref, ref, S_P2X + i, R_P2X + i, self.xto(sign)).start()
        elif op == "recv":
            self.wait_recv(self.shard(self.z + d, self.x + 4 - sign * (s + 1), 0), R_P2X + i)
        else:
            self.wait_send(self.shard(self.z, self.x, 0), S_P2X + i)

    def p2z(self, op, sign, s, d):
        i = (0 if sign > 0 else 16) + s * 4 + d
        if op == "send":
            ref = self.shard(self.z + 8 - sign * s, self.x + d, 1)
            self.remote(ref, ref, S_P2Z + i, R_P2Z + i, self.zto(sign)).start()
        elif op == "recv":
            self.wait_recv(self.shard(self.z + 8 - sign * (s + 1), self.x + d, 1), R_P2Z + i)
        else:
            self.wait_send(self.shard(self.z, self.x, 1), S_P2Z + i)

    def p2z_pairs(self, s):
        if s < 3:
            return [(sign, d) for d in range(4) for sign in (1, -1)]
        return [(1, 0), (1, 1), (-1, 2), (-1, 3)]

    def t_stage(self, n):
        if n == 0:
            self.ts_wait()
            for sign in (1, -1):
                self.p1z("send", sign, 0)
                self.p1x("send", sign, 0)
        elif n == 1:
            for sign in (1, -1):
                self.p1z("recv", sign, 0)
                self.p1z("send", sign, 1)
                self.p1x("recv", sign, 0)
            self.p1x("send", 1, 1)
            for d in (0, 1, 7):
                for sign in (1, -1):
                    self.p2x("send", sign, 0, d)
        elif n == 2:
            for sign in (1, -1):
                self.p1z("recv", sign, 1)
                self.p1z("send", sign, 2)
            self.p1x("recv", 1, 1)
            for sign, d in self.p2z_pairs(0):
                self.p2z("send", sign, 0, d)
            for d in (2, 6):
                for sign in (1, -1):
                    self.p2x("send", sign, 0, d)
        elif n == 3:
            for sign in (1, -1):
                self.p1z("recv", sign, 2)
            self.p1z("send", 1, 3)
            for d in (3, 5):
                for sign in (1, -1):
                    self.p2x("send", sign, 0, d)
        elif n == 4:
            self.p1z("recv", 1, 3)
            for sign in (1, -1):
                self.p2x("send", sign, 0, 4)
            for sign, d in self.p2z_pairs(0):
                self.p2z("recv", sign, 0, d)
                self.p2z("send", sign, 1, d)
        elif n == 5:
            self.p2x_pass((0, 1, 7))
        elif n == 6:
            for sign, d in self.p2z_pairs(1):
                self.p2z("recv", sign, 1, d)
                self.p2z("send", sign, 2, d)
        elif n == 7:
            self.p2x_pass((2, 6))
        elif n == 8:
            last = self.p2z_pairs(3)
            for sign, d in self.p2z_pairs(2):
                self.p2z("recv", sign, 2, d)
                if (sign, d) in last:
                    self.p2z("send", sign, 3, d)
        elif n == 9:
            self.p2x_pass((3, 5, 4))
        elif n == 10:
            for d in Z_ORDER:
                self.p2x("recv", 1 if d % 2 == 0 else -1, 1, d)
            for sign, d in self.p2z_pairs(3):
                self.p2z("recv", sign, 3, d)

    def p2x_pass(self, ds):
        for d in ds:
            for sign in (1, -1):
                self.p2x("recv", sign, 0, d)
            self.p2x("send", 1 if d % 2 == 0 else -1, 1, d)

    def t_finish(self):
        self.ts_finish()
        for s in range(4):
            self.p1z("sent", 1, s)
        for s in range(3):
            self.p1z("sent", -1, s)
        self.p1x("sent", 1, 0)
        self.p1x("sent", 1, 1)
        self.p1x("sent", -1, 0)
        for d in range(8):
            self.p2x("sent", 1, 0, d)
            self.p2x("sent", -1, 0, d)
            self.p2x("sent", 1 if d % 2 == 0 else -1, 1, d)
        for s in range(4):
            for sign, d in self.p2z_pairs(s):
                self.p2z("sent", sign, s, d)


def dot(a, b):
    return jnp.dot(a, b, precision=HI, preferred_element_type=F32)


def dot_t(a, b):
    return lax.dot_general(a, b, (((0,), (0,)), ((), ())), precision=HI, preferred_element_type=F32)


def factor128(buf, ns, hook):
    width = buf.shape[1]
    rows = lax.broadcasted_iota(jnp.int32, (ns, 128), 0)
    for s in range(128 // ns):
        base = s * ns
        strip = [buf[base : base + ns, g * 128 : (g + 1) * 128] for g in range(width // 128)]
        cols = [jnp.broadcast_to(strip[0][:, base + j : base + j + 1], (ns, 128)) for j in range(ns)]
        for p in range(ns):
            r = lax.rsqrt(cols[p][p : p + 1, :])
            low = jnp.where(rows > p, cols[p], 0.0) * r
            for g in range(width // 128):
                u = strip[g][p : p + 1, :] * r
                buf[base + p : base + p + 1, g * 128 : (g + 1) * 128] = u
                strip[g] = strip[g] - low * u
            for j in range(p + 1, ns):
                cols[j] = cols[j] - low * (cols[j][p : p + 1, :] * r)
        nxt = base + ns
        if nxt < 128:
            u = buf[base:nxt, :]
            buf[nxt:128, :] = buf[nxt:128, :] - dot_t(u[:, nxt:128], u)
        hook(nxt)


def chol512(wk, buf, ns, hook):
    eye = (lax.broadcasted_iota(jnp.int32, (128, 128), 0) == lax.broadcasted_iota(jnp.int32, (128, 128), 1)).astype(F32)
    r5 = lax.broadcasted_iota(jnp.int32, (512, 512), 0)
    c5 = lax.broadcasted_iota(jnp.int32, (512, 512), 1)
    wk[:, 512:1024] = (r5 == c5).astype(F32)

    def step(kb, carry):
        off = pl.multiple_of(kb * 128, 128)
        buf[:, 0:128] = wk[pl.ds(off, 128), pl.ds(off, 128)]
        buf[:, 128:256] = eye
        factor128(buf, ns, functools.partial(hook, kb))
        new = dot(buf[:, 128:256], wk[pl.ds(off, 128), :])
        wk[pl.ds(off, 128), :] = new
        wk[pl.ds(off, 128), pl.ds(off, 128)] = buf[:, 0:128]

        def upd(j, c):
            o = pl.multiple_of(j * 128, 128)
            left = wk[pl.ds(off, 128), pl.ds(o, 128)]
            wk[pl.ds(o, 128), :] = wk[pl.ds(o, 128), :] - dot_t(left, wk[pl.ds(off, 128), :])
            return c

        lax.fori_loop(kb + 1, 4, upd, 0)
        return carry

    lax.fori_loop(0, 4, step, 0)


def column_solve(cm, c_ref, w_ref, u_ref, z_ref):
    lanes = pl.ds(pl.multiple_of(cm.k * 256, 256), 256)
    row = lax.broadcasted_iota(jnp.int32, (B, 256), 0)
    eye = (row == lax.broadcasted_iota(jnp.int32, (B, 256), 1) + cm.k * 256).astype(F32)
    col = jnp.zeros((B, 256), jnp.int32) + cm.q
    y0 = dot(w_ref[0], c_ref[0:512, lanes])
    y1 = dot(w_ref[1], c_ref[512:1024, lanes] - dot_t(u_ref[2], y0))
    y0 = jnp.where(col >= 2, y0, jnp.where(col == 0, eye, 0.0))
    y1 = jnp.where(col >= 2, y1, jnp.where(col == 1, eye, 0.0))
    z1 = dot_t(w_ref[1], y1)
    z_ref[512:1024, lanes] = z1
    z_ref[0:512, lanes] = dot_t(w_ref[0], y0 - dot(u_ref[2], z1))


def fused_kernel(m_ref, t_ref, zh_ref, zl_ref, u_ref, w_ref, c_ref, a_ref, z_ref, wk, buf, ssem, rsem, lsem):
    cm = Comm(m_ref, t_ref, c_ref, a_ref, ssem, rsem, lsem)
    refs = cm.factors(w_ref, u_ref)
    cm.load()
    cm.barrier()
    cm.ts_send()
    cm.c_start()

    @pl.when(cm.k == 1)
    def _():
        cm.a_relay(1)
        cm.a_relay(2)
        for n in range(10):
            cm.t_stage(n)
            if n in (2, 5):
                cm.c_pass(n // 4)
        for n, ref in enumerate(refs):
            cm.wait_recv(ref, R_W + n)

    @pl.when(cm.k == 0)
    def _():
        cm.a_relay(0)
        factor(cm, refs, a_ref, w_ref, u_ref, wk, buf)

    cm.c_finish()
    column_solve(cm, c_ref, w_ref, u_ref, z_ref)
    cm.t_stage(10)
    mine = z_ref.at[:, pl.ds(pl.multiple_of(cm.k * 256, 256), 256)]
    theirs = z_ref.at[:, pl.ds(pl.multiple_of(256 - cm.k * 256, 256), 256)]
    cm.remote(mine, mine, S_W + 4, R_W + 4, cm.other).start()
    cm.a_finish()
    cm.t_finish()

    @pl.when(cm.k == 0)
    def _():
        for n, ref in enumerate(refs):
            cm.wait_send(ref, S_W + n)

    cm.wait_send(mine, S_W + 4)
    cm.wait_recv(theirs, R_W + 4)
    zh_ref[...], zl_ref[...] = split(z_ref[...])


def factor(cm, refs, a_ref, w_ref, u_ref, wk, buf):
    def rest():
        cm.a_take(1)
        cm.a_take(2)

    T = lambda n: (functools.partial(cm.t_stage, n),)
    C = lambda n: (functools.partial(cm.c_pass, n),)
    R = (rest,)
    plan = [
        T(0),
        T(1),
        T(2),
        T(3),
        C(0) + T(4),
        (),
        T(5),
        R,
        T(6) + C(1),
        T(7),
        (),
        T(8),
        (),
        T(9),
        (),
        (),
    ]
    upper = lax.broadcasted_iota(jnp.int32, (512, 512), 0) <= lax.broadcasted_iota(jnp.int32, (512, 512), 1)

    def half(h, c):
        @pl.when(h == 0)
        def _():
            wk[:, 0:512] = a_ref[0]

        @pl.when(h == 1)
        def _():
            u01 = lax.dot_general(w_ref[0], a_ref[1], (((1,), (1,)), ((), ())), precision=HI, preferred_element_type=F32)
            u_ref[2] = u01
            wk[:, 0:512] = a_ref[2] - dot_t(u01, u01)

        def hook(kb, done):
            if done % 64:
                return
            for i in range(8):
                acts = plan[2 * i + done // 64 - 1]
                if acts:

                    @pl.when(h * 4 + kb == i)
                    def _():
                        for act in acts:
                            act()

        chol512(wk, buf, NS, hook)
        u_ref[h] = jnp.where(upper, wk[:, 0:512], 0.0)
        w_ref[h] = wk[:, 512:1024]
        return c

    lax.fori_loop(0, 2, half, 0)
    for n in range(4):
        cm.give(refs, n)


def fused(m):
    vm = pl.BlockSpec(memory_space=pltpu.VMEM)
    return pl.pallas_call(
        fused_kernel,
        out_shape=(
            jax.ShapeDtypeStruct((1024, 2048), F32),
            jax.ShapeDtypeStruct((1024, 512), BF16),
            jax.ShapeDtypeStruct((1024, 512), BF16),
            jax.ShapeDtypeStruct((3, 512, 512), F32),
        ),
        in_specs=[pl.BlockSpec(memory_space=pl.ANY)],
        out_specs=(vm,) * 4,
        scratch_shapes=[
            pltpu.VMEM((2, 512, 512), F32),
            pltpu.VMEM((1024, 512), F32),
            pltpu.VMEM((3, 512, 512), F32),
            pltpu.VMEM((1024, 512), F32),
            pltpu.VMEM((512, 1024), F32),
            pltpu.VMEM((128, 256), F32),
            pltpu.SemaphoreType.DMA((N_SEND,)),
            pltpu.SemaphoreType.DMA((N_RECV,)),
            pltpu.SemaphoreType.DMA((3,)),
        ],
        compiler_params=pltpu.CompilerParams(
            collective_id=0, has_side_effects=True, vmem_limit_bytes=50 * 2**20
        ),
    )(m)


def split(v):
    hi = v.astype(BF16)
    return hi, (v - hi.astype(F32)).astype(BF16)


def dot3(a, b, dims):
    (ah, al), (bh, bl) = a, b
    d = functools.partial(lax.dot_general, dimension_numbers=(dims, ((), ())), preferred_element_type=F32)
    return d(al, bh) + d(ah, bl) + d(ah, bh)


NN = ((1,), (0,))
TN = ((0,), (0,))


def update_kernel(f_ref, t_ref, zh_ref, zl_ref, u_ref, o_ref):
    a = pl.program_id(0)
    row = lax.axis_index("row")
    col = lax.axis_index("col") * 4 + lax.axis_index("depth")
    block = a * 8 + row

    @pl.when(block > jnp.minimum(col, 1))
    def _():
        s = dot3(split(t_ref[...]), (zh_ref[...], zl_ref[...]), TN)
        trailing = jnp.zeros((B, B), jnp.int32) + col >= 2
        o_ref[0] = jnp.where(trailing, f_ref[0] - s, s)

    @pl.when(block < jnp.minimum(col, 2))
    def _():
        o_ref[0] = jnp.zeros((B, B), F32)

    @pl.when((block == col) & (col < 2))
    def _():
        o_ref[0] = u_ref[jnp.minimum(col, 1)].T


def update(f, t, zh, zl, u):
    whole = lambda *shape: pl.BlockSpec(shape, lambda a: (0,) * len(shape))
    return pl.pallas_call(
        update_kernel,
        grid=(4,),
        out_shape=jax.ShapeDtypeStruct((4, B, B), F32),
        in_specs=[
            pl.BlockSpec((1, B, B), lambda a: (a, 0, 0)),
            pl.BlockSpec((1024, B), lambda a: (0, a)),
            whole(1024, B),
            whole(1024, B),
            whole(2, B, B),
        ],
        out_specs=pl.BlockSpec((1, B, B), lambda a: (a, 0, 0)),
        compiler_params=pltpu.CompilerParams(
            dimension_semantics=("arbitrary",), vmem_limit_bytes=50 * 2**20
        ),
    )(f, t, zh, zl, u)


def body(matrix):
    return update(matrix[:, 0], *fused(matrix))[:, None]


def solution(mesh):
    spec = P(None, "row", None, ("col", "depth"))
    return jax.shard_map(body, mesh=mesh, in_specs=(spec,), out_specs=spec, check_vma=False)
```

```python
import functools
import jax
import jax.numpy as jnp
from jax import lax
from jax.experimental import pallas as pl
from jax.experimental.pallas import tpu as pltpu
from jax.sharding import PartitionSpec as P

HI = lax.Precision.HIGHEST
F32 = jnp.float32
BF16 = jnp.bfloat16
MESH = pl.DeviceIdType.MESH
B = 512
ROW_SPLIT = 24
NS = 16
Z_ORDER = (0, 1, 7, 2, 6, 3, 5, 4)

R_TS = 0
R_CR = 4
R_CS = 12
R_A0 = 20
R_A1 = 36
R_A2 = 44
R_P1Z = 52
R_P1X = 60
R_P2X = 64
R_P2Z = 96
R_W = 128
N_RECV = 134
S_TS = 0
S_CR = 16
S_CS = 24
S_A = 32
S_P1Z = 256
S_P1X = 264
S_P2X = 268
S_P2Z = 300
S_W = 332
N_SEND = 338


class Comm:
    def __init__(self, m_ref, tbuf, cbuf, abuf, ssem, rsem, lsem):
        self.m, self.t, self.c, self.a = m_ref, tbuf, cbuf, abuf
        self.ssem, self.rsem, self.lsem = ssem, rsem, lsem
        self.r = lax.axis_index("row")
        self.z = lax.axis_index("col")
        self.x = lax.axis_index("depth")
        self.y = self.r // 2
        self.k = self.r % 2
        self.q = self.z * 4 + self.x
        self.other = self.coord(row=self.r + 1 - 2 * self.k)

    def coord(self, row=None, z=None, x=None):
        return {
            "row": self.r if row is None else row,
            "col": self.z if z is None else z,
            "depth": self.x if x is None else x,
        }

    def remote(self, src, dst, ssem, rsem, to):
        return pltpu.make_async_remote_copy(
            src_ref=src,
            dst_ref=dst,
            send_sem=self.ssem.at[ssem],
            recv_sem=self.rsem.at[rsem],
            device_id=to,
            device_id_type=MESH,
        )

    def wait_recv(self, ref, rsem):
        self.remote(ref, ref, 0, rsem, self.other).wait_recv()

    def wait_send(self, ref, ssem):
        self.remote(ref, ref, ssem, 0, self.other).wait_send()

    def barrier(self):
        sem = pltpu.get_barrier_semaphore()
        r, z, x, y, k, q = self.r, self.z, self.x, self.y, self.k, self.q
        ring = [
            self.coord(row=r + 1 - 2 * k),
            self.coord(row=(r + 2) % 8),
            self.coord(row=(r + 6) % 8),
            self.coord(z=(z + 1) % 8),
            self.coord(z=(z + 7) % 8),
            self.coord(x=(x + 1) % 4),
            self.coord(x=(x + 3) % 4),
        ]
        for to in ring:
            pl.semaphore_signal(sem, inc=1, device_id=to, device_id_type=MESH)
        mine = r == q // 16
        for a in range(4):
            col = 8 * a + r

            @pl.when(jnp.logical_not(mine & (col == q)))
            def _():
                to = self.coord(row=q // 16, z=col // 4, x=col % 4)
                pl.semaphore_signal(sem, inc=1, device_id=to, device_id_type=MESH)

        source = r < 2
        dest = q % 8

        @pl.when(source)
        def _():
            def one(i, carry):
                p = r * 16 + i

                @pl.when(jnp.logical_not((dest == r) & (p == q)))
                def _():
                    to = self.coord(row=dest, z=p // 4, x=p % 4)
                    pl.semaphore_signal(sem, inc=1, device_id=to, device_id_type=MESH)

                return carry

            lax.fori_loop(0, 16, one, 0)

        self.own = mine & (q % 8 == r)
        own = self.own.astype(jnp.int32)
        pl.semaphore_wait(sem, 11 - own + source.astype(jnp.int32) * (16 - own))

    def chunk_c(self, k, i):
        return self.c.at[pl.ds(pl.multiple_of(k * B + i * 64, 64), 64), :]

    def load(self):
        @pl.when(self.r < 2)
        def _():
            dst = self.c.at[pl.ds(pl.multiple_of(self.k * B, B), B), :]
            cp = pltpu.make_async_copy(self.m.at[0, 0], dst, self.lsem.at[0])
            cp.start()
            for b, (xs, ks) in enumerate(((0, 0), (0, 1), (1, 1))):

                @pl.when((self.z == 0) & (self.x == xs) & (self.k == ks))
                def _():
                    ca = pltpu.make_async_copy(self.m.at[0, 0], self.a.at[b], self.lsem.at[1])
                    ca.start()
                    ca.wait()

            cp.wait()

    def ts_piece(self, p, a):
        return self.t.at[pl.ds(pl.multiple_of(p * 32, 32), 32), pl.ds(pl.multiple_of(a * B, B), B)]

    def ts_send(self):
        @pl.when(self.r < 2)
        def _():
            dest = self.q % 8
            a = self.q // 8

            def one(i, carry):
                p = self.r * 16 + i
                src = self.c.at[pl.ds(pl.multiple_of(p * 32, 32), 32), :]
                dst = self.ts_piece(p, a)
                is_own = (dest == self.r) & (p == self.q)

                @pl.when(jnp.logical_not(is_own))
                def _():
                    to = self.coord(row=dest, z=p // 4, x=p % 4)
                    self.remote(src, dst, S_TS + i, R_TS + a, to).start()

                @pl.when(is_own)
                def _():
                    pltpu.make_async_copy(src, dst, self.lsem.at[2]).start()

                return carry

            lax.fori_loop(0, 16, one, 0)

    def ts_wait(self):
        for a in range(4):
            own = self.own & (self.q // 8 == a)

            @pl.when(jnp.logical_not(own))
            def _():
                self.wait_recv(self.ts_piece(self.q, a), R_TS + a)

            @pl.when(own)
            def _():
                ref = self.ts_piece(self.q, a)
                pltpu.make_async_copy(ref, ref, self.lsem.at[2]).wait()

    def ts_finish(self):
        @pl.when(self.r < 2)
        def _():
            dest = self.q % 8

            def one(i, carry):
                p = self.r * 16 + i

                @pl.when(jnp.logical_not((dest == self.r) & (p == self.q)))
                def _():
                    self.wait_send(self.ts_piece(0, 0), S_TS + i)

                return carry

            lax.fori_loop(0, 16, one, 0)

    def c_start(self):
        @pl.when(self.y == 0)
        def _():
            self.c_move(0)
            self.c_move(1)

    def c_pass(self, n):
        @pl.when(self.y % 2 == 1)
        def _():
            self.c_move(n)

        if n == 0:

            @pl.when(self.y == 2)
            def _():
                self.c_move(0)
                self.c_move(1)

    def c_move(self, n):
        far = self.y // 3
        h = far if n == 0 else 1 - far
        on = jnp.where(h == 0, self.y != 3, self.y != 1)
        row = (self.r + 2 + 4 * h) % 8

        def one(j, carry):
            i = h * 4 + j
            ref = self.chunk_c(self.k, i)

            @pl.when(self.y != 0)
            def _():
                self.wait_recv(ref, R_CR + i)

            @pl.when(on)
            def _():
                self.remote(ref, ref, S_CR + i, R_CR + i, self.coord(row=row)).start()

            self.remote(ref, ref, S_CS + i, R_CS + i, self.other).start()
            return carry

        lax.fori_loop(0, 4, one, 0)

    def c_finish(self):
        def one(i, carry):
            self.wait_recv(self.chunk_c(1 - self.k, i), R_CS + i)
            self.wait_send(self.chunk_c(self.k, i), S_CS + i)
            h = i // 4

            @pl.when(jnp.where(h == 0, self.y != 3, self.y != 1))
            def _():
                self.wait_send(self.chunk_c(self.k, i), S_CR + i)

            return carry

        lax.fori_loop(0, 8, one, 0)

    A_INFO = ((0, 0, R_A0, 16, 32, 0), (0, 1, R_A1, 8, 64, 16), (1, 1, R_A2, 8, 64, 24))

    def a_children(self, b):
        xs = self.A_INFO[b][0]
        z, y, x, r = self.z, self.y, self.x, self.r
        dx = (x - xs + 4) % 4
        z0, y0 = z == 0, y == 0
        on_x = y0 if b == 1 else y0 & z0
        on_z = y0 & (dx == 0) if b == 1 else z >= 0
        on_y = z >= 0 if b == 1 else z0
        return (
            (on_z & (z <= 3), self.coord(z=(z + 1) % 8)),
            (on_z & (z0 | (z >= 6)), self.coord(z=(z + 7) % 8)),
            (on_y & (y <= 1), self.coord(row=(r + 2) % 8)),
            (on_y & y0, self.coord(row=(r + 6) % 8)),
            (on_x & (dx <= 1), self.coord(x=(x + 1) % 4)),
            (on_x & (dx == 0), self.coord(x=(x + 3) % 4)),
        ) + (((None, self.other),) if b else ())

    def a_chunk(self, b, g, j):
        n = self.A_INFO[b][4]
        row = pl.multiple_of(g * 128 + j * n, n)
        lane = 0 if b == 1 else g * 128
        return self.a.at[b, pl.ds(row, n), lane:B]

    def a_loop(self, b, groups, fn):
        per = 128 // self.A_INFO[b][4]
        for g in groups:

            def one(j, carry):
                fn(self.a_chunk(b, g, j), g * per + j)
                return carry

            lax.fori_loop(0, per, one, 0)

    def a_relay(self, b, groups=range(4)):
        xs, ks, rs, s0 = self.A_INFO[b][:3] + self.A_INFO[b][5:]

        @pl.when(self.k == ks)
        def _():
            source = (self.z == 0) & (self.y == 0) & (self.x == xs)

            def one(ref, j):
                @pl.when(jnp.logical_not(source))
                def _():
                    self.wait_recv(ref, rs + j)

                for d, (cond, to) in enumerate(self.a_children(b)):
                    copy = self.remote(ref, ref, S_A + (s0 + j) * 7 + d, rs + j, to)
                    if cond is None:
                        copy.start()
                    else:
                        pl.when(cond)(copy.start)

            self.a_loop(b, groups, one)

    def a_take(self, b, groups=range(4)):
        ks, rs = self.A_INFO[b][1:3]

        @pl.when(self.k != ks)
        def _():
            self.a_loop(b, groups, lambda ref, j: self.wait_recv(ref, rs + j))

    def a_finish(self, blocks=range(3)):
        for b in blocks:
            ks, s0 = self.A_INFO[b][1], self.A_INFO[b][5]

            @pl.when(self.k == ks)
            def _():
                def one(ref, j):
                    for d, (cond, _) in enumerate(self.a_children(b)):
                        copy = self.remote(ref, ref, S_A + (s0 + j) * 7 + d, 0, self.other)
                        if cond is None:
                            copy.wait_send()
                        else:
                            pl.when(cond)(copy.wait_send)

                self.a_loop(b, range(4), one)

    def factors(self, w, u):
        return (w.at[0], w.at[1], u.at[2], u.at[1])

    def give(self, refs, n):
        self.remote(refs[n], refs[n], S_W + n, R_W + n, self.other).start()

    def shard(self, z, x, half):
        p = (z % 8) * 4 + x % 4
        if half == 0:
            return self.t.at[pl.ds(pl.multiple_of(p * 32, 8), ROW_SPLIT), :]
        return self.t.at[pl.ds(pl.multiple_of(p * 32 + ROW_SPLIT, 8), 32 - ROW_SPLIT), :]

    def zto(self, sign):
        return self.coord(z=(self.z + 8 + sign) % 8)

    def xto(self, sign):
        return self.coord(x=(self.x + 4 + sign) % 4)

    def p1z(self, op, sign, s):
        i = s if sign > 0 else 4 + s
        if op == "send":
            ref = self.shard(self.z + 8 - sign * s, self.x, 0)
            self.remote(ref, ref, S_P1Z + i, R_P1Z + i, self.zto(sign)).start()
        elif op == "recv":
            self.wait_recv(self.shard(self.z + 8 - sign * (s + 1), self.x, 0), R_P1Z + i)
        else:
            self.wait_send(self.shard(self.z, self.x, 0), S_P1Z + i)

    def p1x(self, op, sign, s):
        i = s if sign > 0 else 2 + s
        if op == "send":
            ref = self.shard(self.z, self.x + 4 - sign * s, 1)
            self.remote(ref, ref, S_P1X + i, R_P1X + i, self.xto(sign)).start()
        elif op == "recv":
            self.wait_recv(self.shard(self.z, self.x + 4 - sign * (s + 1), 1), R_P1X + i)
        else:
            self.wait_send(self.shard(self.z, self.x, 1), S_P1X + i)

    def p2x(self, op, sign, s, d):
        i = (0 if sign > 0 else 16) + s * 8 + d
        if op == "send":
            ref = self.shard(self.z + d, self.x + 4 - sign * s, 0)
            self.remote(ref, ref, S_P2X + i, R_P2X + i, self.xto(sign)).start()
        elif op == "recv":
            self.wait_recv(self.shard(self.z + d, self.x + 4 - sign * (s + 1), 0), R_P2X + i)
        else:
            self.wait_send(self.shard(self.z, self.x, 0), S_P2X + i)

    def p2z(self, op, sign, s, d):
        i = (0 if sign > 0 else 16) + s * 4 + d
        if op == "send":
            ref = self.shard(self.z + 8 - sign * s, self.x + d, 1)
            self.remote(ref, ref, S_P2Z + i, R_P2Z + i, self.zto(sign)).start()
        elif op == "recv":
            self.wait_recv(self.shard(self.z + 8 - sign * (s + 1), self.x + d, 1), R_P2Z + i)
        else:
            self.wait_send(self.shard(self.z, self.x, 1), S_P2Z + i)

    def p2z_pairs(self, s):
        if s < 3:
            return [(sign, d) for d in range(4) for sign in (1, -1)]
        return [(1, 0), (1, 1), (-1, 2), (-1, 3)]

    def t_stage(self, n):
        if n == 0:
            self.ts_wait()
            for sign in (1, -1):
                self.p1z("send", sign, 0)
                self.p1x("send", sign, 0)
        elif n == 1:
            for sign in (1, -1):
                self.p1z("recv", sign, 0)
                self.p1z("send", sign, 1)
                self.p1x("recv", sign, 0)
            self.p1x("send", 1, 1)
            for d in (0, 1, 7):
                for sign in (1, -1):
                    self.p2x("send", sign, 0, d)
        elif n == 2:
            for sign in (1, -1):
                self.p1z("recv", sign, 1)
                self.p1z("send", sign, 2)
            self.p1x("recv", 1, 1)
            for sign, d in self.p2z_pairs(0):
                self.p2z("send", sign, 0, d)
            for d in (2, 6):
                for sign in (1, -1):
                    self.p2x("send", sign, 0, d)
        elif n == 3:
            for sign in (1, -1):
                self.p1z("recv", sign, 2)
            self.p1z("send", 1, 3)
            for d in (3, 5):
                for sign in (1, -1):
                    self.p2x("send", sign, 0, d)
        elif n == 4:
            self.p1z("recv", 1, 3)
            for sign in (1, -1):
                self.p2x("send", sign, 0, 4)
            for sign, d in self.p2z_pairs(0):
                self.p2z("recv", sign, 0, d)
                self.p2z("send", sign, 1, d)
        elif n == 5:
            self.p2x_pass((0, 1, 7))
        elif n == 6:
            for sign, d in self.p2z_pairs(1):
                self.p2z("recv", sign, 1, d)
                self.p2z("send", sign, 2, d)
        elif n == 7:
            self.p2x_pass((2, 6))
        elif n == 8:
            last = self.p2z_pairs(3)
            for sign, d in self.p2z_pairs(2):
                self.p2z("recv", sign, 2, d)
                if (sign, d) in last:
                    self.p2z("send", sign, 3, d)
        elif n == 9:
            self.p2x_pass((3, 5, 4))
        elif n == 10:
            for d in Z_ORDER:
                self.p2x("recv", 1 if d % 2 == 0 else -1, 1, d)
            for sign, d in self.p2z_pairs(3):
                self.p2z("recv", sign, 3, d)

    def p2x_pass(self, ds):
        for d in ds:
            for sign in (1, -1):
                self.p2x("recv", sign, 0, d)
            self.p2x("send", 1 if d % 2 == 0 else -1, 1, d)

    def t_finish(self):
        self.ts_finish()
        for s in range(4):
            self.p1z("sent", 1, s)
        for s in range(3):
            self.p1z("sent", -1, s)
        self.p1x("sent", 1, 0)
        self.p1x("sent", 1, 1)
        self.p1x("sent", -1, 0)
        for d in range(8):
            self.p2x("sent", 1, 0, d)
            self.p2x("sent", -1, 0, d)
            self.p2x("sent", 1 if d % 2 == 0 else -1, 1, d)
        for s in range(4):
            for sign, d in self.p2z_pairs(s):
                self.p2z("sent", sign, s, d)


def dot(a, b):
    return jnp.dot(a, b, precision=HI, preferred_element_type=F32)


def dot_t(a, b):
    return lax.dot_general(a, b, (((0,), (0,)), ((), ())), precision=HI, preferred_element_type=F32)


def factor128(buf, ns, hook):
    width = buf.shape[1]
    rows = lax.broadcasted_iota(jnp.int32, (ns, 128), 0)
    for s in range(128 // ns):
        base = s * ns
        strip = [buf[base : base + ns, g * 128 : (g + 1) * 128] for g in range(width // 128)]
        cols = [jnp.broadcast_to(strip[0][:, base + j : base + j + 1], (ns, 128)) for j in range(ns)]
        for p in range(ns):
            r = lax.rsqrt(cols[p][p : p + 1, :])
            low = jnp.where(rows > p, cols[p], 0.0) * r
            for g in range(width // 128):
                u = strip[g][p : p + 1, :] * r
                buf[base + p : base + p + 1, g * 128 : (g + 1) * 128] = u
                strip[g] = strip[g] - low * u
            for j in range(p + 1, ns):
                cols[j] = cols[j] - low * (cols[j][p : p + 1, :] * r)
        nxt = base + ns
        if nxt < 128:
            u = buf[base:nxt, :]
            buf[nxt:128, :] = buf[nxt:128, :] - dot_t(u[:, nxt:128], u)
        hook(nxt)


def chol512(wk, buf, ns, hook):
    eye = (lax.broadcasted_iota(jnp.int32, (128, 128), 0) == lax.broadcasted_iota(jnp.int32, (128, 128), 1)).astype(F32)
    r5 = lax.broadcasted_iota(jnp.int32, (512, 512), 0)
    c5 = lax.broadcasted_iota(jnp.int32, (512, 512), 1)
    wk[:, 512:1024] = (r5 == c5).astype(F32)

    def step(kb, carry):
        off = pl.multiple_of(kb * 128, 128)
        buf[:, 0:128] = wk[pl.ds(off, 128), pl.ds(off, 128)]
        buf[:, 128:256] = eye
        factor128(buf, ns, functools.partial(hook, kb))
        new = dot(buf[:, 128:256], wk[pl.ds(off, 128), :])
        wk[pl.ds(off, 128), :] = new
        wk[pl.ds(off, 128), pl.ds(off, 128)] = buf[:, 0:128]

        def upd(j, c):
            o = pl.multiple_of(j * 128, 128)
            left = wk[pl.ds(off, 128), pl.ds(o, 128)]
            wk[pl.ds(o, 128), :] = wk[pl.ds(o, 128), :] - dot_t(left, wk[pl.ds(off, 128), :])
            return c

        lax.fori_loop(kb + 1, 4, upd, 0)
        return carry

    lax.fori_loop(0, 4, step, 0)


def column_solve(cm, c_ref, w_ref, u_ref, z_ref):
    lanes = pl.ds(pl.multiple_of(cm.k * 256, 256), 256)
    row = lax.broadcasted_iota(jnp.int32, (B, 256), 0)
    eye = (row == lax.broadcasted_iota(jnp.int32, (B, 256), 1) + cm.k * 256).astype(F32)
    col = jnp.zeros((B, 256), jnp.int32) + cm.q
    y0 = dot(w_ref[0], c_ref[0:512, lanes])
    y1 = dot(w_ref[1], c_ref[512:1024, lanes] - dot_t(u_ref[2], y0))
    y0 = jnp.where(col >= 2, y0, jnp.where(col == 0, eye, 0.0))
    y1 = jnp.where(col >= 2, y1, jnp.where(col == 1, eye, 0.0))
    z1 = dot_t(w_ref[1], y1)
    z_ref[512:1024, lanes] = z1
    z_ref[0:512, lanes] = dot_t(w_ref[0], y0 - dot(u_ref[2], z1))


def fused_kernel(m_ref, t_ref, zh_ref, zl_ref, u_ref, w_ref, c_ref, a_ref, z_ref, wk, buf, ssem, rsem, lsem):
    cm = Comm(m_ref, t_ref, c_ref, a_ref, ssem, rsem, lsem)
    refs = cm.factors(w_ref, u_ref)
    cm.load()
    cm.barrier()
    cm.ts_send()
    cm.c_start()

    @pl.when(cm.k == 1)
    def _():
        cm.a_relay(1)
        cm.a_relay(2)
        for n in range(10):
            cm.t_stage(n)
            if n in (2, 5):
                cm.c_pass(n // 4)
        for n, ref in enumerate(refs):
            cm.wait_recv(ref, R_W + n)

    @pl.when(cm.k == 0)
    def _():
        cm.a_relay(0)
        factor(cm, refs, a_ref, w_ref, u_ref, wk, buf)

    cm.c_finish()
    column_solve(cm, c_ref, w_ref, u_ref, z_ref)
    cm.t_stage(10)
    mine = z_ref.at[:, pl.ds(pl.multiple_of(cm.k * 256, 256), 256)]
    theirs = z_ref.at[:, pl.ds(pl.multiple_of(256 - cm.k * 256, 256), 256)]
    cm.remote(mine, mine, S_W + 4, R_W + 4, cm.other).start()
    cm.a_finish()
    cm.t_finish()

    @pl.when(cm.k == 0)
    def _():
        for n, ref in enumerate(refs):
            cm.wait_send(ref, S_W + n)

    cm.wait_send(mine, S_W + 4)
    cm.wait_recv(theirs, R_W + 4)
    zh_ref[...], zl_ref[...] = split(z_ref[...])


def factor(cm, refs, a_ref, w_ref, u_ref, wk, buf):
    def rest():
        cm.a_take(1)
        cm.a_take(2)

    T = lambda n: (functools.partial(cm.t_stage, n),)
    C = lambda n: (functools.partial(cm.c_pass, n),)
    R = (rest,)
    plan = [
        T(0),
        (),
        T(1),
        (),
        T(2),
        (),
        T(3) + C(0),
        R,
        T(4),
        T(5) + C(1),
        (),
        T(6),
        (),
        T(7),
        T(8),
        T(9),
    ]
    upper = lax.broadcasted_iota(jnp.int32, (512, 512), 0) <= lax.broadcasted_iota(jnp.int32, (512, 512), 1)

    def half(h, c):
        @pl.when(h == 0)
        def _():
            wk[:, 0:512] = a_ref[0]

        @pl.when(h == 1)
        def _():
            u01 = lax.dot_general(w_ref[0], a_ref[1], (((1,), (1,)), ((), ())), precision=HI, preferred_element_type=F32)
            u_ref[2] = u01
            wk[:, 0:512] = a_ref[2] - dot_t(u01, u01)

        def hook(kb, done):
            if done % 64:
                return
            for i in range(8):
                acts = plan[2 * i + done // 64 - 1]
                if acts:

                    @pl.when(h * 4 + kb == i)
                    def _():
                        for act in acts:
                            act()

        chol512(wk, buf, NS, hook)
        u_ref[h] = jnp.where(upper, wk[:, 0:512], 0.0)
        w_ref[h] = wk[:, 512:1024]
        return c

    lax.fori_loop(0, 2, half, 0)
    for n in range(4):
        cm.give(refs, n)


def fused(m):
    vm = pl.BlockSpec(memory_space=pltpu.VMEM)
    return pl.pallas_call(
        fused_kernel,
        out_shape=(
            jax.ShapeDtypeStruct((1024, 2048), F32),
            jax.ShapeDtypeStruct((1024, 512), BF16),
            jax.ShapeDtypeStruct((1024, 512), BF16),
            jax.ShapeDtypeStruct((3, 512, 512), F32),
        ),
        in_specs=[pl.BlockSpec(memory_space=pl.ANY)],
        out_specs=(vm,) * 4,
        scratch_shapes=[
            pltpu.VMEM((2, 512, 512), F32),
            pltpu.VMEM((1024, 512), F32),
            pltpu.VMEM((3, 512, 512), F32),
            pltpu.VMEM((1024, 512), F32),
            pltpu.VMEM((512, 1024), F32),
            pltpu.VMEM((128, 256), F32),
            pltpu.SemaphoreType.DMA((N_SEND,)),
            pltpu.SemaphoreType.DMA((N_RECV,)),
            pltpu.SemaphoreType.DMA((3,)),
        ],
        compiler_params=pltpu.CompilerParams(
            collective_id=0, has_side_effects=True, vmem_limit_bytes=50 * 2**20
        ),
    )(m)


def split(v):
    hi = v.astype(BF16)
    return hi, (v - hi.astype(F32)).astype(BF16)


def dot3(a, b, dims):
    (ah, al), (bh, bl) = a, b
    d = functools.partial(lax.dot_general, dimension_numbers=(dims, ((), ())), preferred_element_type=F32)
    return d(al, bh) + d(ah, bl) + d(ah, bh)


NN = ((1,), (0,))
TN = ((0,), (0,))


def update_kernel(f_ref, t_ref, zh_ref, zl_ref, u_ref, o_ref):
    a = pl.program_id(0)
    row = lax.axis_index("row")
    col = lax.axis_index("col") * 4 + lax.axis_index("depth")
    block = a * 8 + row

    @pl.when(block > jnp.minimum(col, 1))
    def _():
        s = dot3(split(t_ref[...]), (zh_ref[...], zl_ref[...]), TN)
        trailing = jnp.zeros((B, B), jnp.int32) + col >= 2
        o_ref[0] = jnp.where(trailing, f_ref[0] - s, s)

    @pl.when(block < jnp.minimum(col, 2))
    def _():
        o_ref[0] = jnp.zeros((B, B), F32)

    @pl.when((block == col) & (col < 2))
    def _():
        o_ref[0] = u_ref[jnp.minimum(col, 1)].T


def update(f, t, zh, zl, u):
    whole = lambda *shape: pl.BlockSpec(shape, lambda a: (0,) * len(shape))
    return pl.pallas_call(
        update_kernel,
        grid=(4,),
        out_shape=jax.ShapeDtypeStruct((4, B, B), F32),
        in_specs=[
            pl.BlockSpec((1, B, B), lambda a: (a, 0, 0)),
            pl.BlockSpec((1024, B), lambda a: (0, a)),
            whole(1024, B),
            whole(1024, B),
            whole(2, B, B),
        ],
        out_specs=pl.BlockSpec((1, B, B), lambda a: (a, 0, 0)),
        compiler_params=pltpu.CompilerParams(
            dimension_semantics=("arbitrary",), vmem_limit_bytes=50 * 2**20
        ),
    )(f, t, zh, zl, u)


def body(matrix):
    return update(matrix[:, 0], *fused(matrix))[:, None]


def solution(mesh):
    spec = P(None, "row", None, ("col", "depth"))
    return jax.shard_map(body, mesh=mesh, in_specs=(spec,), out_specs=spec, check_vma=False)
```
